128 devices in a mesh: lat: 16 (over z, y), lon: 8 (over x, core).
Axes of the slice: x: 4, y: 4, z: 4, core: 2. Of those that a mesh axis runs over, the one named last changes fastest.
Arguments:
- grid_feat: bfloat16 [131072, 512], P(('lat', 'lon')), may hold values from -6 to 6
- mesh_feat: bfloat16 [8192, 512], P(('lat', 'lon')), may hold values from -6 to 6
- enc_send: int32 [128, 9, 256], P(('lat', 'lon')), may hold values from 0 to 1023
- enc_recv: int32 [128, 9, 256], P(('lat', 'lon')), may hold values from 0 to 63
- enc_count: int32 [128, 9], P(('lat', 'lon')), may hold values from 0 to 256, as said below
- dec_send: int32 [128, 9, 512], P(('lat', 'lon')), may hold values from 0 to 63
- dec_recv: int32 [128, 9, 512], P(('lat', 'lon')), may hold values from 0 to 1023
- dec_count: int32 [128, 9], P(('lat', 'lon')), may hold values from 0 to 512, as said below
- enc_src: bfloat16 [512, 512], replicated, may hold values from -0.25 to 0.25
- enc_dst: bfloat16 [512, 512], replicated, may hold values from -0.25 to 0.25
- enc_bias: float32 [512], replicated, may hold values from -3 to 3
- enc_out: bfloat16 [512, 512], replicated, may hold values from -0.03125 to 0.03125
- dec_src: bfloat16 [512, 512], replicated, may hold values from -0.25 to 0.25
- dec_dst: bfloat16 [512, 512], replicated, may hold values from -0.25 to 0.25
- dec_bias: float32 [512], replicated, may hold values from -3 to 3
- dec_out: bfloat16 [512, 512], replicated, may hold values from -0.1875 to 0.1875
- grid_cot: bfloat16 [131072, 512], P(('lat', 'lon')), may hold values from -6 to 6
Outputs:
- grid_new: bfloat16 [131072, 512], P(('lat', 'lon'))
- mesh_grad: bfloat16 [8192, 512], P(('lat', 'lon'))
- grid_grad: bfloat16 [131072, 512], P(('lat', 'lon'))
The draws below stay inside these ranges and needn't reach their ends.
Inputs may be any that keep to these rules, and one draw needn't show every extreme that they name: `enc_send`: row of the grid device's own tile. `enc_recv`: row of the mesh tile of the block's neighbour. `enc_count`: live slots of each block; 0 where the neighbour would lie beyond a pole; block 4 (the device itself) is full, and in every draw some device receives full blocks from all its neighbours. `dec_send`: row of the mesh tile of the block's neighbour. `dec_recv`: row of the grid device's own tile. `dec_count`: live slots of each block; 0 where the neighbour would lie beyond a pole; block 4 (the device itself) is full, and in every draw some device sends full blocks to all its neighbours.
All inputs are finite; a program needn't handle non-finite values.
Results may differ from the reference program's by a relative error of at most 0.0086.
Values may be sent and summed in bfloat16 or wider, within the bound.
No kernel may reach another device: no remote copies, remote signals or barrier semaphores. Data moves between devices by JAX's collectives and lax.ppermute only.
A program may use at most 128 MiB of HBM per device.

```python
import jax
import jax.numpy as jnp
from jax import lax

D = 512
G_DEV = 1024
M_DEV = 64
CAP_E = 256
CAP_D = 512
OWNERS = 128
GRID = 131072
MESH = 8192
N_LAT = 16
N_LON = 8


def neighbour_counts(key, capacity):
    owners = jnp.arange(OWNERS, dtype=jnp.int32)
    offsets = jnp.arange(9, dtype=jnp.int32)
    lat_band = owners // N_LON
    lon_sector = owners % N_LON
    target_band = lat_band[:, None] + offsets[None, :] // 3 - 1
    target_sector = (lon_sector[:, None] + offsets[None, :] % 3 - 1) % N_LON
    inside = (target_band >= 0) & (target_band < N_LAT)
    target = jnp.clip(target_band, 0, N_LAT - 1) * N_LON + target_sector
    polar_band = (lat_band == 0) | (lat_band == N_LAT - 1)
    quiet_key, busy_key, busiest_key = jax.random.split(key, 3)
    quiet_load = jax.random.randint(quiet_key, (OWNERS, 9), capacity // 4, 3 * capacity // 4 + 1)
    busy_load = jax.random.randint(busy_key, (OWNERS, 9), capacity // 2, capacity + 1)
    counts = jnp.where(polar_band[:, None], busy_load, quiet_load)
    busiest = jax.random.randint(busiest_key, (), 0, OWNERS)
    filled = (offsets[None, :] == 4) | (target == busiest)
    counts = jnp.where(filled, capacity, counts)
    counts = jnp.where(inside, counts, 0)
    return counts.astype(jnp.int32)


def draw_enc_count(key, part):
    return neighbour_counts(jax.random.fold_in(key, 11), CAP_E)


def draw_dec_count(key, part):
    return neighbour_counts(jax.random.fold_in(key, 23), CAP_D)


def with_ends(result, own_key, least, high):
    spot = [jax.random.randint(jax.random.fold_in(own_key, axis), (), 0, length) for axis, length in enumerate(result.shape)]
    longest = result.shape.index(max(result.shape))
    neighbour = spot[:longest] + [(spot[longest] + 1) % result.shape[longest]] + spot[longest + 1:]
    return result.at[tuple(spot)].set(least).at[tuple(neighbour)].set(high)


def steps_of(stream_key, extent, cuts, least, largest):
    gain = 1.0
    for axis_at, shards_of in cuts:
        steps = jax.random.uniform(jax.random.fold_in(jax.random.fold_in(stream_key, 6), axis_at), (shards_of,), jnp.float32, least / len(cuts), largest / len(cuts))
        gain = gain * jnp.repeat(jnp.exp(steps), extent[axis_at] // shards_of).reshape((-1,) + (1,) * (len(extent) - 1 - axis_at))
    return gain


def normal_values(rng, dims, scale, bound, shards=(), kind=jnp.bfloat16):
    factor_of = steps_of(rng, dims, shards, -0.22, 0.18) if shards else 1.0
    values = jax.random.normal(rng, dims, jnp.float32) * scale * factor_of
    return jnp.minimum(jnp.maximum(values, -bound), bound).astype(kind)


def setup_inputs(seed: int = 0) -> dict:
    splits = jax.random.split(jax.random.key(seed), 18)
    return {
        "grid_feat": normal_values(splits[0], (GRID, D), 1.0, 6.0, ((0, 128),)),
        "mesh_feat": normal_values(splits[1], (MESH, D), 1.0, 6.0, ((0, 128),)),
        "enc_send": with_ends(jax.random.randint(splits[2], (OWNERS, 9, CAP_E), 0, G_DEV), jax.random.fold_in(splits[2], 1), 0, G_DEV - 1).astype(jnp.int32),
        "enc_recv": with_ends(jax.random.randint(splits[3], (OWNERS, 9, CAP_E), 0, M_DEV), jax.random.fold_in(splits[3], 1), 0, M_DEV - 1).astype(jnp.int32),
        "enc_count": draw_enc_count(jax.random.fold_in(splits[17], 71), 0),
        "dec_send": with_ends(jax.random.randint(splits[5], (OWNERS, 9, CAP_D), 0, M_DEV), jax.random.fold_in(splits[5], 1), 0, M_DEV - 1).astype(jnp.int32),
        "dec_recv": with_ends(jax.random.randint(splits[6], (OWNERS, 9, CAP_D), 0, G_DEV), jax.random.fold_in(splits[6], 1), 0, G_DEV - 1).astype(jnp.int32),
        "dec_count": draw_dec_count(jax.random.fold_in(splits[17], 71), 0),
        "enc_src": normal_values(splits[8], (D, D), D ** -0.5, 0.25),
        "enc_dst": normal_values(splits[9], (D, D), D ** -0.5, 0.25),
        "enc_bias": normal_values(splits[10], (D,), 0.5, 3.0, (), jnp.float32),
        "enc_out": normal_values(splits[11], (D, D), (D * 64) ** -0.5, 0.03125),
        "dec_src": normal_values(splits[12], (D, D), D ** -0.5, 0.25),
        "dec_dst": normal_values(splits[13], (D, D), D ** -0.5, 0.25),
        "dec_bias": normal_values(splits[14], (D,), 0.5, 3.0, (), jnp.float32),
        "dec_out": normal_values(splits[15], (D, D), (D * 2) ** -0.5, 0.1875),
        "grid_cot": normal_values(splits[16], (GRID, D), 1.0, 6.0, ((0, 128),)),
    }


def silu_slope(pre_act):
    squashed = jax.nn.sigmoid(pre_act)
    return squashed * (1.0 + pre_act * (1.0 - squashed))


def slot_keep(counts, capacity):
    slot_index = jnp.arange(capacity, dtype=jnp.int32)
    return (slot_index[None, :] < counts[:, None]).astype(jnp.float32)[..., None]


def rounded(values):
    return lax.optimization_barrier(values.astype(jnp.bfloat16)).astype(jnp.float32)


def neighbour_owners():
    owners = jnp.arange(OWNERS, dtype=jnp.int32)
    offsets = jnp.arange(9, dtype=jnp.int32)
    lat_band = owners // N_LON
    lon_sector = owners % N_LON
    target_band = jnp.clip(lat_band[:, None] + offsets[None, :] // 3 - 1, 0, N_LAT - 1)
    target_sector = (lon_sector[:, None] + offsets[None, :] % 3 - 1) % N_LON
    return (target_band * N_LON + target_sector).astype(jnp.int32)


def reference(grid_feat, mesh_feat, enc_send, enc_recv, enc_count, dec_send, dec_recv, dec_count, enc_src, enc_dst, enc_bias, enc_out, dec_src, dec_dst, dec_bias, dec_out, grid_cot):
    owners = jnp.arange(OWNERS, dtype=jnp.int32)
    neighbours = neighbour_owners()
    enc_proj = jnp.dot(grid_feat, enc_src, preferred_element_type=jnp.float32).astype(jnp.bfloat16).reshape(OWNERS, G_DEV, D)
    mesh_side = jnp.dot(mesh_feat, enc_dst, preferred_element_type=jnp.float32)

    def enc_edges(device):
        senders = enc_proj[device][enc_send[device]]
        receivers = (neighbours[device][:, None] * M_DEV + enc_recv[device]).astype(jnp.int32)
        pre_act = senders.astype(jnp.float32) + mesh_side[receivers] + enc_bias
        return pre_act, slot_keep(enc_count[device], CAP_E), receivers

    def enc_forward(running, device):
        pre_act, keeper, receivers = enc_edges(device)
        flat_msg = rounded(jax.nn.silu(pre_act) * keeper).reshape(-1, D)
        return running.at[receivers.reshape(-1)].add(flat_msg), None

    enc_total, _ = lax.scan(enc_forward, jnp.zeros((MESH, D), jnp.float32), owners)
    enc_sum = enc_total.astype(jnp.bfloat16)
    mesh_new = (mesh_feat.astype(jnp.float32) + jnp.dot(enc_sum, enc_out, preferred_element_type=jnp.float32)).astype(jnp.bfloat16)

    dec_proj = jnp.dot(mesh_new, dec_src, preferred_element_type=jnp.float32).astype(jnp.bfloat16)
    grid_side = jnp.dot(grid_feat, dec_dst, preferred_element_type=jnp.float32).reshape(OWNERS, G_DEV, D)

    def dec_edges(device):
        senders = (neighbours[device][:, None] * M_DEV + dec_send[device]).astype(jnp.int32)
        receivers = dec_recv[device]
        pre_act = dec_proj[senders].astype(jnp.float32) + grid_side[device][receivers] + dec_bias
        return pre_act, slot_keep(dec_count[device], CAP_D), senders, receivers

    def dec_forward(device):
        pre_act, keeper, senders, receivers = dec_edges(device)
        flat_msg = rounded(jax.nn.silu(pre_act) * keeper).reshape(-1, D)
        summed = jax.ops.segment_sum(flat_msg, receivers.reshape(-1), num_segments=G_DEV)
        return summed.astype(jnp.bfloat16)

    dec_sum = lax.map(dec_forward, owners).reshape(GRID, D)
    grid_new = (grid_feat.astype(jnp.float32) + jnp.dot(dec_sum, dec_out, preferred_element_type=jnp.float32)).astype(jnp.bfloat16)

    grid_back = jnp.dot(grid_cot, dec_out.T, preferred_element_type=jnp.float32).astype(jnp.bfloat16).reshape(OWNERS, G_DEV, D)

    def dec_backward(running, device):
        pre_act, keeper, senders, receivers = dec_edges(device)
        flat_grad = rounded(grid_back[device][receivers].astype(jnp.float32) * silu_slope(pre_act) * keeper).reshape(-1, D)
        local_sum = jax.ops.segment_sum(flat_grad, receivers.reshape(-1), num_segments=G_DEV).astype(jnp.bfloat16)
        return running.at[senders.reshape(-1)].add(flat_grad), local_sum

    mesh_total, dec_local = lax.scan(dec_backward, jnp.zeros((MESH, D), jnp.float32), owners)
    dec_grid = jnp.dot(dec_local.reshape(GRID, D), dec_dst.T, preferred_element_type=jnp.float32)
    mesh_back = jnp.dot(mesh_total.astype(jnp.bfloat16), dec_src.T, preferred_element_type=jnp.float32)
    enc_back = jnp.dot(mesh_back.astype(jnp.bfloat16), enc_out.T, preferred_element_type=jnp.float32).astype(jnp.bfloat16)

    def enc_backward(running, device):
        pre_act, keeper, receivers = enc_edges(device)
        flat_grad = rounded(enc_back[receivers].astype(jnp.float32) * silu_slope(pre_act) * keeper).reshape(-1, D)
        local_sum = jax.ops.segment_sum(flat_grad, enc_send[device].reshape(-1), num_segments=G_DEV).astype(jnp.bfloat16)
        return running.at[receivers.reshape(-1)].add(flat_grad), local_sum

    enc_local, grid_total = lax.scan(enc_backward, jnp.zeros((MESH, D), jnp.float32), owners)
    mesh_grad = (mesh_back + jnp.dot(enc_local.astype(jnp.bfloat16), enc_dst.T, preferred_element_type=jnp.float32)).astype(jnp.bfloat16)
    enc_grid = jnp.dot(grid_total.reshape(GRID, D), enc_src.T, preferred_element_type=jnp.float32)
    grid_grad = (grid_cot.astype(jnp.float32) + dec_grid + enc_grid).astype(jnp.bfloat16)
    return grid_new, mesh_grad, grid_grad
```

```python
import jax
import jax.numpy as jnp
from jax import lax
from jax.experimental import pallas as pl
from jax.experimental.pallas import tpu as pltpu
from jax.sharding import PartitionSpec as P

F32 = jnp.float32
BF16 = jnp.bfloat16
LANES = 128
CHUNK = 256

VMEM = pl.BlockSpec(memory_space=pltpu.VMEM)
SMEM = pl.BlockSpec(memory_space=pltpu.SMEM)
ANY = pl.BlockSpec(memory_space=pl.ANY)


def mm(lhs, rhs):
    return jnp.dot(lhs, rhs, preferred_element_type=F32)


def mm_nt(lhs, rhs):
    return lax.dot_general(lhs, rhs, (((1,), (1,)), ((), ())), preferred_element_type=F32)


def as_hot(mask):
    return jnp.where(mask, 1.0, 0.0).astype(BF16)


def down_rows(index_row):
    return jnp.transpose(jnp.broadcast_to(index_row, (LANES, index_row.shape[1])))


def gather_hot(index_row, rows):
    spread = down_rows(index_row)
    lane = lax.broadcasted_iota(jnp.int32, spread.shape, 1)
    return jnp.concatenate(
        [as_hot(spread == lane + start) for start in range(0, rows, LANES)], axis=1
    )


def scatter_hot(index_row, rows, live):
    slots = index_row.shape[1]
    slot = lax.broadcasted_iota(jnp.int32, (1, slots), 1)
    index_row = jnp.where(slot < live, index_row, -1)
    return as_hot(lax.broadcasted_iota(jnp.int32, (rows, slots), 0) == index_row)


def gate(pre):
    return 0.5 * jnp.tanh(0.5 * pre) + 0.5


def chunks_of(live):
    return lax.div(live + (CHUNK - 1), CHUNK)


def chunk_at(c):
    return pl.multiple_of(c * CHUNK, CHUNK)


def block_of(step, flip):
    lon_place = lax.div(step, 3)
    slot = lax.rem(step, 3)
    first = 1 - 2 * flip
    lat_offset = jnp.where(slot == 0, 0, jnp.where(slot == 1, first, -first))
    return 3 * (lat_offset + 1) + lon_place


def enc_gather_kernel(counts, send, feat, weight, out, proj):
    k = pl.program_id(0)

    @pl.when(k == 0)
    def _():
        proj[...] = mm(feat[...], weight[...]).astype(BF16)

    @pl.when(counts[0, k] > 0)
    def _():
        hot = gather_hot(send[pl.ds(k, 1), :], proj.shape[0])
        out[0] = mm(hot, proj[...]).astype(BF16)


def dec_gather_kernel(counts, recv, feat, cot, weight, out_weight, bias, out, table):
    k = pl.program_id(0)
    width = feat.shape[1]

    @pl.when(k == 0)
    def _():
        table[:, :width] = (mm(feat[...], weight[...]) + bias[...]).astype(BF16)
        table[:, width:] = mm_nt(cot[...], out_weight[...]).astype(BF16)

    live = counts[0, k]
    for start in range(0, recv.shape[1], CHUNK):

        @pl.when(live > start)
        def _():
            hot = gather_hot(recv[pl.ds(k, 1), pl.ds(start, CHUNK)], table.shape[0])
            out[0, start : start + CHUNK, :] = mm(hot, table[...]).astype(BF16)


def start_if(live, copy):
    @pl.when(live > 0)
    def _():
        copy.start()


def wait_if(live, copy):
    @pl.when(live > 0)
    def _():
        copy.wait()


def enc_forward_kernel(
    counts, flip, recv, left, own, right, weight, bias, sent,
    out_left, out_own, out_right, slope,
    near, side, sent_in, slope_out, partial, near_sem, in_sem, out_sem, part_sem,
):
    odd = flip[0]
    rows = near.shape[2]
    steps = 9
    near_in = [
        pltpu.make_async_copy(ref, near.at[b], near_sem.at[b])
        for b, ref in enumerate((left, own, right))
    ]
    for copy in near_in:
        copy.start()

    def block_in(k):
        return pltpu.make_async_copy(sent.at[k], sent_in.at[k], in_sem.at[k])

    def block_out(k):
        return pltpu.make_async_copy(slope_out.at[k], slope.at[k], out_sem.at[k])

    @pl.loop(0, steps)
    def _(i):
        k = block_of(i, odd)
        start_if(counts[0, k], block_in(k))

    for copy in near_in:
        copy.wait()
    feats = near[...].reshape(steps * rows, near.shape[3])
    exact = mm(feats, weight[...]) + bias[...]
    high = exact.astype(BF16)
    low = (exact - high.astype(F32)).astype(BF16)
    side[:, :rows, :] = high.reshape(steps, rows, -1)
    side[:, rows:, :] = low.reshape(steps, rows, -1)

    @pl.loop(0, steps)
    def _(i):
        k = block_of(i, odd)
        live = counts[0, k]
        partial[i] = jnp.zeros(partial.shape[1:], BF16)

        @pl.when(live > 0)
        def _():
            index_row = recv[pl.ds(k, 1), :]
            spread = down_rows(index_row)
            lane = lax.broadcasted_iota(jnp.int32, spread.shape, 1)
            hot = as_hot(spread == jnp.where(lane < rows, lane, lane - rows))
            received = mm(hot, side[i])
            block_in(k).wait()
            pre = sent_in[k].astype(F32) + received
            squashed = gate(pre)
            message = pre * squashed
            slope_out[k] = (squashed + message * (1.0 - squashed)).astype(BF16)
            block_out(k).start()
            total = mm(scatter_hot(index_row, rows, live), message.astype(BF16))
            partial[i] = total.astype(BF16)

    send_partials(partial, (out_left, out_own, out_right), part_sem)

    @pl.loop(0, steps)
    def _(k):
        wait_if(counts[0, k], block_out(k))


def send_partials(partial, outs, sems):
    copies = [
        pltpu.make_async_copy(partial.at[pl.ds(3 * b, 3)], ref, sems.at[b])
        for b, ref in enumerate(outs)
    ]
    for copy in copies:
        copy.start()
    for copy in copies:
        copy.wait()


def dec_kernel(
    counts, flip, send, left, own, right, table,
    out_left, out_own, out_right, results,
    near, table_in, results_out, partial, total, near_sem, in_sem, out_sem, part_sem,
):
    odd = flip[0]
    rows = near.shape[2]
    width = near.shape[3]
    steps = 9
    near_in = [
        pltpu.make_async_copy(ref, near.at[b], near_sem.at[b])
        for b, ref in enumerate((left, own, right))
    ]
    for copy in near_in:
        copy.start()

    def block_in(k):
        return pltpu.make_async_copy(table.at[k], table_in.at[k], in_sem.at[k])

    def block_out(k):
        return pltpu.make_async_copy(results_out.at[k], results.at[k], out_sem.at[k])

    @pl.loop(0, steps)
    def _(i):
        k = block_of(i, odd)
        start_if(counts[0, k], block_in(k))

    for copy in near_in:
        copy.wait()

    @pl.loop(0, steps)
    def _(i):
        k = block_of(i, odd)
        live = counts[0, k]
        wait_if(live, block_in(k))
        total[...] = jnp.zeros(total.shape, F32)
        tile = near[lax.div(i, 3), lax.rem(i, 3)]

        @pl.loop(0, chunks_of(live))
        def _(c):
            at = chunk_at(c)
            index_row = send[pl.ds(k, 1), pl.ds(at, CHUNK)]
            spread = down_rows(index_row)
            lane = lax.broadcasted_iota(jnp.int32, spread.shape, 1)
            hot = as_hot(spread == lane)[:, :rows]
            received = mm(hot, tile)
            pre = table_in[k, pl.ds(at, CHUNK), :width].astype(F32) + received
            squashed = gate(pre)
            message = pre * squashed
            results_out[k, pl.ds(at, CHUNK), :width] = message.astype(BF16)
            slope = squashed + message * (1.0 - squashed)
            grad = (table_in[k, pl.ds(at, CHUNK), width:].astype(F32) * slope).astype(BF16)
            results_out[k, pl.ds(at, CHUNK), width:] = grad
            total[...] += mm(scatter_hot(index_row, rows, live - at), grad)

        start_if(live, block_out(k))
        partial[i] = total[...].astype(BF16)

    send_partials(partial, (out_left, out_own, out_right), part_sem)

    @pl.loop(0, steps)
    def _(k):
        wait_if(counts[0, k], block_out(k))


def enc_backward_kernel(
    counts, flip, recv, left, own, right, slope,
    out_left, out_own, out_right, grads,
    near, slope_in, grads_out, partial, near_sem, in_sem, out_sem, part_sem,
):
    odd = flip[0]
    rows = near.shape[2]
    steps = 9
    near_in = [
        pltpu.make_async_copy(ref, near.at[b], near_sem.at[b])
        for b, ref in enumerate((left, own, right))
    ]
    for copy in near_in:
        copy.start()

    def block_in(k):
        return pltpu.make_async_copy(slope.at[k], slope_in.at[k], in_sem.at[k])

    def block_out(k):
        return pltpu.make_async_copy(grads_out.at[k], grads.at[k], out_sem.at[k])

    @pl.loop(0, steps)
    def _(i):
        k = block_of(i, odd)
        start_if(counts[0, k], block_in(k))

    for copy in near_in:
        copy.wait()

    @pl.loop(0, steps)
    def _(i):
        k = block_of(i, odd)
        live = counts[0, k]
        partial[i] = jnp.zeros(partial.shape[1:], BF16)

        @pl.when(live > 0)
        def _():
            index_row = recv[pl.ds(k, 1), :]
            spread = down_rows(index_row)
            lane = lax.broadcasted_iota(jnp.int32, spread.shape, 1)
            hot = as_hot(spread == lane)[:, :rows]
            received = mm(hot, near[lax.div(i, 3), lax.rem(i, 3)])
            block_in(k).wait()
            grad = (received * slope_in[k].astype(F32)).astype(BF16)
            grads_out[k] = grad
            block_out(k).start()
            partial[i] = mm(scatter_hot(index_row, rows, live), grad).astype(BF16)

    send_partials(partial, (out_left, out_own, out_right), part_sem)

    @pl.loop(0, steps)
    def _(k):
        wait_if(counts[0, k], block_out(k))


def dec_scatter_kernel(counts, recv, results, feat, out_weight, grid_new, local, total):
    k = pl.program_id(0)
    width = feat.shape[1]

    @pl.when(k == 0)
    def _():
        total[...] = jnp.zeros(total.shape, F32)

    live = counts[0, k]
    for start in range(0, recv.shape[1], CHUNK):

        @pl.when(live > start)
        def _():
            index_row = recv[pl.ds(k, 1), pl.ds(start, CHUNK)]
            hot = scatter_hot(index_row, total.shape[0], live - start)
            total[...] += mm(hot, results[0, start : start + CHUNK, :])

    @pl.when(k == pl.num_programs(0) - 1)
    def _():
        summed = total[:, :width].astype(BF16)
        grid_new[...] = (feat[...].astype(F32) + mm(summed, out_weight[...])).astype(BF16)
        local[...] = total[:, width:].astype(BF16)


def enc_scatter_kernel(counts, send, grads, cot, local, dec_weight, enc_weight, out, total):
    k = pl.program_id(0)

    @pl.when(k == 0)
    def _():
        total[...] = jnp.zeros(total.shape, F32)

    live = counts[0, k]

    @pl.when(live > 0)
    def _():
        hot = scatter_hot(send[pl.ds(k, 1), :], total.shape[0], live)
        total[...] += mm(hot, grads[0])

    @pl.when(k == pl.num_programs(0) - 1)
    def _():
        back = mm_nt(local[...], dec_weight[...])
        back += mm_nt(total[...].astype(BF16), enc_weight[...])
        out[...] = (cot[...].astype(F32) + back).astype(BF16)


def whole(shape):
    return pl.BlockSpec(shape, lambda k: (0,) * len(shape))


def per_block(shape):
    return pl.BlockSpec((1,) + shape, lambda k: (k, 0, 0))


def along(axis, pairs):
    return lambda value: lax.ppermute(value, axis, pairs)


def lat_pairs(size, start):
    edges = [(i, (i + 1) % size) for i in range(start, size, 2)]
    return edges + [(j, i) for i, j in edges]


def on_device(
    grid_feat, mesh_feat, enc_send, enc_recv, enc_count, dec_send, dec_recv, dec_count,
    enc_src, enc_dst, enc_bias, enc_out, dec_src, dec_dst, dec_bias, dec_out, grid_cot,
):
    grid_rows, width = grid_feat.shape
    mesh_rows = mesh_feat.shape[0]
    cap_e = enc_send.shape[2]
    cap_d = dec_send.shape[2]
    lat_size = lax.axis_size("lat")
    lon_size = lax.axis_size("lon")
    flip = lax.rem(lax.axis_index("lat"), 2).astype(jnp.int32).reshape(1)
    first = along("lat", lat_pairs(lat_size, 0))
    second = along("lat", lat_pairs(lat_size, 1))
    east = along("lon", [(i, (i + 1) % lon_size) for i in range(lon_size)])
    west = along("lon", [((i + 1) % lon_size, i) for i in range(lon_size)])

    def spread(tile):
        three = jnp.stack([tile, first(tile), second(tile)])
        return east(three), three, west(three)

    def fold(left, own, right):
        from_east = west(left).astype(F32)
        from_west = east(right).astype(F32)
        three = own.astype(F32) + from_east + from_west
        sent = three[1:].astype(BF16)
        return three[0] + first(sent[0]).astype(F32) + second(sent[1]).astype(F32)

    def kernel(body, out_shape, **settings):
        return pl.pallas_call(
            body,
            out_shape=out_shape,
            compiler_params=pltpu.CompilerParams(vmem_limit_bytes=56 * 1024 * 1024),
            **settings,
        )

    def array(*shape):
        return jax.ShapeDtypeStruct(shape, BF16)

    three = array(3, mesh_rows, width)
    partial_sems = [
        pltpu.SemaphoreType.DMA((3,)),
        pltpu.SemaphoreType.DMA((9,)),
        pltpu.SemaphoreType.DMA((9,)),
        pltpu.SemaphoreType.DMA((3,)),
    ]
    near_scratch = pltpu.VMEM((3, 3, mesh_rows, width), BF16)
    partial_scratch = pltpu.VMEM((9, mesh_rows, width), BF16)

    enc_send, enc_recv, dec_send, dec_recv = (
        a[0] for a in (enc_send, enc_recv, dec_send, dec_recv)
    )

    near_feat = spread(mesh_feat)
    sent = kernel(
        enc_gather_kernel,
        array(9, cap_e, width),
        grid=(9,),
        in_specs=[SMEM, whole((9, cap_e)), whole((grid_rows, width)), whole((width, width))],
        out_specs=per_block((cap_e, width)),
        scratch_shapes=[pltpu.VMEM((grid_rows, width), BF16)],
        name="enc_gather",
    )(enc_count, enc_send, grid_feat, enc_src)
    table = kernel(
        dec_gather_kernel,
        array(9, cap_d, 2 * width),
        grid=(9,),
        in_specs=[
            SMEM, whole((9, cap_d)), whole((grid_rows, width)), whole((grid_rows, width)),
            whole((width, width)), whole((width, width)), whole((1, width)),
        ],
        out_specs=per_block((cap_d, 2 * width)),
        scratch_shapes=[pltpu.VMEM((grid_rows, 2 * width), BF16)],
        name="dec_gather",
    )(dec_count, dec_recv, grid_feat, grid_cot, dec_dst, dec_out, dec_bias.reshape(1, width))

    *enc_partial, slope = kernel(
        enc_forward_kernel,
        [three, three, three, array(9, cap_e, width)],
        in_specs=[SMEM, SMEM, VMEM, ANY, ANY, ANY, VMEM, VMEM, ANY],
        out_specs=[ANY] * 4,
        scratch_shapes=[
            near_scratch,
            pltpu.VMEM((9, 2 * mesh_rows, width), BF16),
            pltpu.VMEM((9, cap_e, width), BF16),
            pltpu.VMEM((9, cap_e, width), BF16),
            partial_scratch,
            *partial_sems,
        ],
        name="enc_forward",
    )(enc_count, flip, enc_recv, *near_feat, enc_dst, enc_bias.reshape(1, width), sent)
    enc_sum = fold(*enc_partial).astype(BF16)
    mesh_new = (mesh_feat.astype(F32) + mm(enc_sum, enc_out)).astype(BF16)
    dec_proj = mm(mesh_new, dec_src).astype(BF16)

    *dec_partial, results = kernel(
        dec_kernel,
        [three, three, three, array(9, cap_d, 2 * width)],
        in_specs=[SMEM, SMEM, VMEM, ANY, ANY, ANY, ANY],
        out_specs=[ANY] * 4,
        scratch_shapes=[
            near_scratch,
            pltpu.VMEM((9, cap_d, 2 * width), BF16),
            pltpu.VMEM((9, cap_d, 2 * width), BF16),
            partial_scratch,
            pltpu.VMEM((mesh_rows, width), F32),
            *partial_sems,
        ],
        name="dec_edges",
    )(dec_count, flip, dec_send, *spread(dec_proj), table)
    mesh_total = fold(*dec_partial).astype(BF16)
    mesh_back = mm_nt(mesh_total, dec_src)
    enc_back = mm_nt(mesh_back.astype(BF16), enc_out).astype(BF16)

    grid_new, local = kernel(
        dec_scatter_kernel,
        [array(grid_rows, width), array(grid_rows, width)],
        grid=(9,),
        in_specs=[
            SMEM, whole((9, cap_d)), per_block((cap_d, 2 * width)),
            whole((grid_rows, width)), whole((width, width)),
        ],
        out_specs=[whole((grid_rows, width)), whole((grid_rows, width))],
        scratch_shapes=[pltpu.VMEM((grid_rows, 2 * width), F32)],
        name="dec_scatter",
    )(dec_count, dec_recv, results, grid_feat, dec_out)

    *grad_partial, grads = kernel(
        enc_backward_kernel,
        [three, three, three, array(9, cap_e, width)],
        in_specs=[SMEM, SMEM, VMEM, ANY, ANY, ANY, ANY],
        out_specs=[ANY] * 4,
        scratch_shapes=[
            near_scratch,
            pltpu.VMEM((9, cap_e, width), BF16),
            pltpu.VMEM((9, cap_e, width), BF16),
            partial_scratch,
            *partial_sems,
        ],
        name="enc_backward",
    )(enc_count, flip, enc_recv, *spread(enc_back), slope)
    enc_local = fold(*grad_partial).astype(BF16)
    mesh_grad = (mesh_back + mm_nt(enc_local, enc_dst)).astype(BF16)

    grid_grad = kernel(
        enc_scatter_kernel,
        array(grid_rows, width),
        grid=(9,),
        in_specs=[
            SMEM, whole((9, cap_e)), per_block((cap_e, width)), whole((grid_rows, width)),
            whole((grid_rows, width)), whole((width, width)), whole((width, width)),
        ],
        out_specs=whole((grid_rows, width)),
        scratch_shapes=[pltpu.VMEM((grid_rows, width), F32)],
        name="enc_scatter",
    )(enc_count, enc_send, grads, grid_cot, local, dec_dst, enc_src)
    return grid_new, mesh_grad, grid_grad


def solution(mesh):
    rows = P(("lat", "lon"), None)
    edges = P(("lat", "lon"), None, None)
    return jax.shard_map(
        on_device,
        mesh=mesh,
        in_specs=(rows, rows, edges, edges, rows, edges, edges, rows)
        + (P(),) * 8
        + (rows,),
        out_specs=(rows, rows, rows),
        check_vma=False,
    )
```

```python
import jax
import jax.numpy as jnp
from jax import lax
from jax.experimental import pallas as pl
from jax.experimental.pallas import tpu as pltpu
from jax.sharding import PartitionSpec as P

F32 = jnp.float32
BF16 = jnp.bfloat16
LANES = 128
CHUNK = 256

VMEM = pl.BlockSpec(memory_space=pltpu.VMEM)
SMEM = pl.BlockSpec(memory_space=pltpu.SMEM)


def mm(lhs, rhs):
    return jnp.dot(lhs, rhs, preferred_element_type=F32)


def mm_nt(lhs, rhs):
    return lax.dot_general(lhs, rhs, (((1,), (1,)), ((), ())), preferred_element_type=F32)


def as_hot(mask):
    return jnp.where(mask, 1.0, 0.0).astype(BF16)


def down_rows(index_row):
    return jnp.transpose(jnp.broadcast_to(index_row, (LANES, index_row.shape[1])))


def gather_hot(index_row, rows):
    spread = down_rows(index_row)
    lane = lax.broadcasted_iota(jnp.int32, spread.shape, 1)
    return jnp.concatenate(
        [as_hot(spread == lane + start) for start in range(0, rows, LANES)], axis=1
    )


def scatter_hot(index_row, rows, live):
    slots = index_row.shape[1]
    slot = lax.broadcasted_iota(jnp.int32, (1, slots), 1)
    index_row = jnp.where(slot < live, index_row, -1)
    return as_hot(lax.broadcasted_iota(jnp.int32, (rows, slots), 0) == index_row)


def gate(pre):
    return 0.5 * jnp.tanh(0.5 * pre) + 0.5


def chunks_of(live):
    return lax.div(live + (CHUNK - 1), CHUNK)


def chunk_at(c):
    return pl.multiple_of(c * CHUNK, CHUNK)


def block_of(step, flip):
    lon_place = lax.div(step, 3)
    slot = lax.rem(step, 3)
    first = 1 - 2 * flip
    lat_offset = jnp.where(slot == 0, 0, jnp.where(slot == 1, first, -first))
    return 3 * (lat_offset + 1) + lon_place


def enc_gather_kernel(counts, send, feat, weight, out, proj):
    proj[...] = mm(feat[...], weight[...]).astype(BF16)

    @pl.loop(0, send.shape[0])
    def _(k):
        @pl.when(counts[0, k] > 0)
        def _():
            out[k] = mm(gather_hot(send[k], proj.shape[0]), proj[...]).astype(BF16)


def gather_slots(counts, recv, table, out):
    @pl.loop(0, recv.shape[0])
    def _(k):
        @pl.loop(0, chunks_of(counts[0, k]))
        def _(c):
            at = chunk_at(c)
            hot = gather_hot(recv[k, :, pl.ds(at, CHUNK)], table.shape[0])
            out[k, pl.ds(at, CHUNK), :] = mm(hot, table[...]).astype(BF16)


def side_gather_kernel(counts, recv, feat, weight, bias, out, table):
    table[...] = (mm(feat[...], weight[...]) + bias[...]).astype(BF16)
    gather_slots(counts, recv, table, out)


def back_gather_kernel(counts, recv, cot, weight, out, table):
    table[...] = mm_nt(cot[...], weight[...]).astype(BF16)
    gather_slots(counts, recv, table, out)


def near_blocks(flip, body):
    @pl.loop(0, 3)
    def _(slot):
        for place in range(3):
            body(block_of(3 * place + slot, flip[0]), slot, place)


def enc_forward_kernel(
    counts, flip, recv, left, own, right, weight, bias, sent,
    out_left, out_own, out_right, slope, side,
):
    rows = own.shape[1]
    for place, near in enumerate((left, own, right)):
        feats = near[...].reshape(3 * rows, near.shape[2])
        exact = mm(feats, weight[...]) + bias[...]
        high = exact.astype(BF16)
        low = (exact - high.astype(F32)).astype(BF16)
        side[place, :, :rows, :] = high.reshape(3, rows, -1)
        side[place, :, rows:, :] = low.reshape(3, rows, -1)
    outs = (out_left, out_own, out_right)

    def one(k, slot, place):
        live = counts[0, k]
        outs[place][slot] = jnp.zeros(own.shape[1:], BF16)

        @pl.when(live > 0)
        def _():
            index_row = recv[k]
            spread = down_rows(index_row)
            lane = lax.broadcasted_iota(jnp.int32, spread.shape, 1)
            hot = as_hot(spread == jnp.where(lane < rows, lane, lane - rows))
            pre = sent[k].astype(F32) + mm(hot, side[place, slot])
            squashed = gate(pre)
            message = pre * squashed
            slope[k] = (squashed + message * (1.0 - squashed)).astype(BF16)
            total = mm(scatter_hot(index_row, rows, live), message.astype(BF16))
            outs[place][slot] = total.astype(BF16)

    near_blocks(flip, one)


def dec_kernel(
    counts, flip, send, left, own, right, side, back,
    out_left, out_own, out_right, messages, grads, total,
):
    rows = own.shape[1]
    nears = (left, own, right)
    outs = (out_left, out_own, out_right)

    def one(k, slot, place):
        live = counts[0, k]
        total[...] = jnp.zeros(total.shape, F32)

        @pl.loop(0, chunks_of(live))
        def _(c):
            at = chunk_at(c)
            index_row = send[k, :, pl.ds(at, CHUNK)]
            spread = down_rows(index_row)
            lane = lax.broadcasted_iota(jnp.int32, spread.shape, 1)
            hot = as_hot(spread == lane)[:, :rows]
            pre = side[k, pl.ds(at, CHUNK), :].astype(F32) + mm(hot, nears[place][slot])
            squashed = gate(pre)
            message = pre * squashed
            messages[k, pl.ds(at, CHUNK), :] = message.astype(BF16)
            slope = squashed + message * (1.0 - squashed)
            grad = (back[k, pl.ds(at, CHUNK), :].astype(F32) * slope).astype(BF16)
            grads[k, pl.ds(at, CHUNK), :] = grad
            total[...] += mm(scatter_hot(index_row, rows, live - at), grad)

        outs[place][slot] = total[...].astype(BF16)

    near_blocks(flip, one)


def enc_backward_kernel(
    counts, flip, recv, left, own, right, slope, out_left, out_own, out_right, grads
):
    rows = own.shape[1]
    nears = (left, own, right)
    outs = (out_left, out_own, out_right)

    def one(k, slot, place):
        live = counts[0, k]
        outs[place][slot] = jnp.zeros(own.shape[1:], BF16)

        @pl.when(live > 0)
        def _():
            index_row = recv[k]
            spread = down_rows(index_row)
            lane = lax.broadcasted_iota(jnp.int32, spread.shape, 1)
            hot = as_hot(spread == lane)[:, :rows]
            received = mm(hot, nears[place][slot])
            grad = (received * slope[k].astype(F32)).astype(BF16)
            grads[k] = grad
            outs[place][slot] = mm(scatter_hot(index_row, rows, live), grad).astype(BF16)

    near_blocks(flip, one)


def scatter_slots(counts, recv, values, total):
    total[...] = jnp.zeros(total.shape, F32)

    @pl.loop(0, recv.shape[0])
    def _(k):
        live = counts[0, k]

        @pl.loop(0, chunks_of(live))
        def _(c):
            at = chunk_at(c)
            hot = scatter_hot(recv[k, :, pl.ds(at, CHUNK)], total.shape[0], live - at)
            total[...] += mm(hot, values[k, pl.ds(at, CHUNK), :])


def dec_sum_kernel(counts, recv, messages, feat, weight, out, total):
    scatter_slots(counts, recv, messages, total)
    out[...] = (feat[...].astype(F32) + mm(total[...].astype(BF16), weight[...])).astype(BF16)


def dec_local_kernel(counts, recv, grads, out, total):
    scatter_slots(counts, recv, grads, total)
    out[...] = total[...].astype(BF16)


def enc_scatter_kernel(counts, send, grads, cot, local, dec_weight, enc_weight, out, total):
    scatter_slots(counts, send, grads, total)
    back = mm_nt(local[...], dec_weight[...])
    back += mm_nt(total[...].astype(BF16), enc_weight[...])
    out[...] = (cot[...].astype(F32) + back).astype(BF16)


def along(axis, pairs):
    return lambda value: lax.ppermute(value, axis, pairs)


def lat_pairs(size, start):
    edges = [(i, (i + 1) % size) for i in range(start, size, 2)]
    return edges + [(j, i) for i, j in edges]


def on_device(
    grid_feat, mesh_feat, enc_send, enc_recv, enc_count, dec_send, dec_recv, dec_count,
    enc_src, enc_dst, enc_bias, enc_out, dec_src, dec_dst, dec_bias, dec_out, grid_cot,
):
    grid_rows, width = grid_feat.shape
    mesh_rows = mesh_feat.shape[0]
    cap_e = enc_send.shape[2]
    cap_d = dec_send.shape[2]
    lat_size = lax.axis_size("lat")
    lon_size = lax.axis_size("lon")
    flip = lax.rem(lax.axis_index("lat"), 2).astype(jnp.int32).reshape(1)
    first = along("lat", lat_pairs(lat_size, 0))
    second = along("lat", lat_pairs(lat_size, 1))
    east = along("lon", [(i, (i + 1) % lon_size) for i in range(lon_size)])
    west = along("lon", [((i + 1) % lon_size, i) for i in range(lon_size)])

    def spread(tile, name):
        with jax.named_scope(name + "_lat"):
            pieces = [tile, first(tile), second(tile)]
        with jax.named_scope(name + "_lon"):
            three = jnp.stack(pieces)
            return east(three), three, west(three)

    def fold(left, own, right, name):
        with jax.named_scope(name + "_lon"):
            from_east = west(left).astype(F32)
            from_west = east(right).astype(F32)
        three = own.astype(F32) + from_east + from_west
        sent = three[1:].astype(BF16)
        with jax.named_scope(name + "_lat"):
            return three[0] + first(sent[0]).astype(F32) + second(sent[1]).astype(F32)

    def kernel(body, outs, scratch, name, *args, smem=1, mib=12, work=0):
        with jax.named_scope(name):
            return pl.pallas_call(
                body,
                out_shape=outs,
                in_specs=[SMEM] * smem + [VMEM] * (len(args) - smem),
                out_specs=[VMEM] * len(outs),
                scratch_shapes=scratch,
                compiler_params=pltpu.CompilerParams(vmem_limit_bytes=mib * 1024 * 1024),
                cost_estimate=pl.CostEstimate(flops=work, bytes_accessed=0, transcendentals=0),
                name=name,
            )(*args)

    def array(*shape):
        return jax.ShapeDtypeStruct(shape, BF16)

    three = [array(3, mesh_rows, width)] * 3
    enc_slots = [array(9, cap_e, width)]
    dec_slots = [array(9, cap_d, width)]
    grid_tile = [array(grid_rows, width)]
    rounded_grid = [pltpu.VMEM((grid_rows, width), BF16)]
    exact_grid = [pltpu.VMEM((grid_rows, width), F32)]
    enc_work = 2 * grid_rows * width * 9 * cap_e
    dec_work = 2 * grid_rows * width * 9 * cap_d

    enc_send, enc_recv, dec_send, dec_recv = (
        jnp.swapaxes(a, 0, 1) for a in (enc_send, enc_recv, dec_send, dec_recv)
    )

    near_feat = spread(mesh_feat, "e1")
    (sent,) = kernel(
        enc_gather_kernel, enc_slots, rounded_grid, "enc_gather",
        enc_count, enc_send, grid_feat, enc_src, work=enc_work,
    )
    (back_at,) = kernel(
        back_gather_kernel, dec_slots, rounded_grid, "back_gather",
        dec_count, dec_recv, grid_cot, dec_out, work=dec_work,
    )
    (side_at,) = kernel(
        side_gather_kernel, dec_slots, rounded_grid, "side_gather",
        dec_count, dec_recv, grid_feat, dec_dst, dec_bias.reshape(1, width), work=dec_work,
    )

    *enc_partial, slope = kernel(
        enc_forward_kernel, three + enc_slots,
        [pltpu.VMEM((3, 3, 2 * mesh_rows, width), BF16)], "enc_forward",
        enc_count, flip, enc_recv, *near_feat, enc_dst, enc_bias.reshape(1, width), sent,
        smem=2, work=enc_work // 4,
    )
    enc_sum = fold(*enc_partial, "f1").astype(BF16)
    mesh_new = (mesh_feat.astype(F32) + mm(enc_sum, enc_out)).astype(BF16)
    dec_proj = mm(mesh_new, dec_src).astype(BF16)

    *dec_partial, messages, dec_grads = kernel(
        dec_kernel, three + dec_slots * 2, [pltpu.VMEM((mesh_rows, width), F32)], "dec_edges",
        dec_count, flip, dec_send, *spread(dec_proj, "e2"), side_at, back_at,
        smem=2, work=dec_work // 4,
    )
    mesh_total = fold(*dec_partial, "f2").astype(BF16)
    mesh_back = mm_nt(mesh_total, dec_src)
    enc_back = mm_nt(mesh_back.astype(BF16), enc_out).astype(BF16)

    (grid_new,) = kernel(
        dec_sum_kernel, grid_tile, exact_grid, "dec_sum",
        dec_count, dec_recv, messages, grid_feat, dec_out, work=dec_work,
    )
    (local,) = kernel(
        dec_local_kernel, grid_tile, exact_grid, "dec_local",
        dec_count, dec_recv, dec_grads, work=dec_work,
    )

    *grad_partial, grads = kernel(
        enc_backward_kernel, three + enc_slots, [], "enc_backward",
        enc_count, flip, enc_recv, *spread(enc_back, "e3"), slope,
        smem=2, work=enc_work // 4,
    )
    enc_local = fold(*grad_partial, "f3").astype(BF16)
    mesh_grad = (mesh_back + mm_nt(enc_local, enc_dst)).astype(BF16)

    (grid_grad,) = kernel(
        enc_scatter_kernel, grid_tile, exact_grid, "enc_scatter",
        enc_count, enc_send, grads, grid_cot, local, dec_dst, enc_src, work=enc_work,
    )
    return grid_new, mesh_grad, grid_grad


def solution(mesh):
    rows = P(("lat", "lon"), None)
    edges = P(("lat", "lon"), None, None)
    return jax.shard_map(
        on_device,
        mesh=mesh,
        in_specs=(rows, rows, edges, edges, rows, edges, edges, rows)
        + (P(),) * 8
        + (rows,),
        out_specs=(rows, rows, rows),
        check_vma=False,
    )
```

```python
import jax
import jax.numpy as jnp
from jax import lax
from jax.experimental import pallas as pl
from jax.experimental.pallas import tpu as pltpu
from jax.sharding import PartitionSpec as P

F32 = jnp.float32
BF16 = jnp.bfloat16
LANES = 128
CHUNK = 128
GROUP = 4

VMEM = pl.BlockSpec(memory_space=pltpu.VMEM)
SMEM = pl.BlockSpec(memory_space=pltpu.SMEM)


def mm(lhs, rhs):
    return jnp.dot(lhs, rhs, preferred_element_type=F32)


def mm_nt(lhs, rhs):
    return lax.dot_general(lhs, rhs, (((1,), (1,)), ((), ())), preferred_element_type=F32)


def as_hot(mask):
    return jnp.where(mask, 1.0, 0.0).astype(BF16)


def down_rows(index_row):
    return jnp.transpose(jnp.broadcast_to(index_row, (LANES, index_row.shape[1])))


def gather_hot(index_row, rows):
    spread = down_rows(index_row)
    lane = lax.broadcasted_iota(jnp.int32, spread.shape, 1)
    return jnp.concatenate(
        [as_hot(spread == lane + start) for start in range(0, rows, LANES)], axis=1
    )


def scatter_hot(index_row, rows, live):
    slots = index_row.shape[1]
    slot = lax.broadcasted_iota(jnp.int32, (1, slots), 1)
    index_row = jnp.where(slot < live, index_row, -1)
    return as_hot(lax.broadcasted_iota(jnp.int32, (rows, slots), 0) == index_row)


def gate(pre):
    return 0.5 * jnp.tanh(0.5 * pre) + 0.5


def list_chunks(counts, capacity, block, start, live):
    found = jnp.int32(0)
    for k in range(counts.shape[1]):
        count = counts[0, k]
        for at in range(0, capacity, CHUNK):
            block[found] = k
            start[found] = at
            live[found] = count - at
            found += (count > at).astype(jnp.int32)
    for j in range(GROUP - 1):
        block[found + j] = counts.shape[1] // 2
        start[found + j] = 0
        live[found + j] = 0
    return lax.div(found + (GROUP - 1), GROUP)


def each_group(groups, chunk_list, body):
    block, start, live = chunk_list

    @pl.loop(0, groups)
    def _(g):
        at = [GROUP * g + j for j in range(GROUP)]
        body([(block[n], pl.multiple_of(start[n], CHUNK), live[n]) for n in at])


def rows_of(index_ref, chunk):
    k, at, _ = chunk
    return index_ref[k, :, pl.ds(at, CHUNK)]


def place_of(k, flip):
    lat_offset = lax.div(k, 3) - 1
    first = 1 - 2 * flip
    slot = jnp.where(lat_offset == 0, 0, jnp.where(lat_offset == first, 1, 2))
    return 3 * lax.rem(k, 3) + slot


def gather_slots(counts, index_ref, table, out, chunk_list):
    groups = list_chunks(counts, index_ref.shape[2], *chunk_list)

    def body(chunks):
        hots = [gather_hot(rows_of(index_ref, c), table.shape[0]) for c in chunks]
        rows = mm(jnp.concatenate(hots, axis=0), table[...]).astype(BF16)
        for j, (k, at, _) in enumerate(chunks):
            out[k, pl.ds(at, CHUNK), :] = rows[j * CHUNK : (j + 1) * CHUNK]

    each_group(groups, chunk_list, body)


def enc_gather_kernel(counts, send, feat, weight, out, table, *chunk_list):
    table[...] = mm(feat[...], weight[...]).astype(BF16)
    gather_slots(counts, send, table, out, chunk_list)


def side_gather_kernel(counts, recv, feat, weight, bias, out, table, *chunk_list):
    table[...] = (mm(feat[...], weight[...]) + bias[...]).astype(BF16)
    gather_slots(counts, recv, table, out, chunk_list)


def back_gather_kernel(counts, recv, cot, weight, out, table, *chunk_list):
    table[...] = mm_nt(cot[...], weight[...]).astype(BF16)
    gather_slots(counts, recv, table, out, chunk_list)


def near_hot(index_row, rows):
    spread = down_rows(index_row)
    lane = lax.broadcasted_iota(jnp.int32, spread.shape, 1)
    return as_hot(spread == jnp.where(lane < rows, lane, lane - rows))


def edge_groups(counts, index_ref, flip, side, total, outs, chunk_list, edges):
    rows = total.shape[1]
    groups = list_chunks(counts, index_ref.shape[2], *chunk_list)
    total[...] = jnp.zeros(total.shape, F32)

    def body(chunks):
        for chunk in chunks:
            k, _, live = chunk
            place = place_of(k, flip[0])
            index_row = rows_of(index_ref, chunk)
            received = mm(near_hot(index_row, rows)[:, : side.shape[1]], side[place])
            value = edges(chunk, received)
            total[place] += mm(scatter_hot(index_row, rows, live), value)

    each_group(groups, chunk_list, body)
    for place, out in enumerate(outs):
        out[...] = total[3 * place : 3 * place + 3].astype(BF16)


def enc_forward_kernel(
    counts, flip, recv, left, own, right, weight, bias, sent,
    out_left, out_own, out_right, slope, side, total, *chunk_list,
):
    rows = own.shape[1]
    for place, near in enumerate((left, own, right)):
        feats = near[...].reshape(3 * rows, near.shape[2])
        exact = mm(feats, weight[...]) + bias[...]
        high = exact.astype(BF16)
        low = (exact - high.astype(F32)).astype(BF16)
        side[3 * place : 3 * place + 3, :rows, :] = high.reshape(3, rows, -1)
        side[3 * place : 3 * place + 3, rows:, :] = low.reshape(3, rows, -1)

    def edges(chunk, received):
        k, at, _ = chunk
        pre = sent[k, pl.ds(at, CHUNK), :].astype(F32) + received
        squashed = gate(pre)
        message = pre * squashed
        slope[k, pl.ds(at, CHUNK), :] = (squashed + message * (1.0 - squashed)).astype(BF16)
        return message.astype(BF16)

    outs = (out_left, out_own, out_right)
    edge_groups(counts, recv, flip, side, total, outs, chunk_list, edges)


def dec_kernel(
    counts, flip, send, left, own, right, side, back,
    out_left, out_own, out_right, messages, grads, near, total, *chunk_list,
):
    for place, tiles in enumerate((left, own, right)):
        near[3 * place : 3 * place + 3] = tiles[...]

    def edges(chunk, received):
        k, at, _ = chunk
        here = (k, pl.ds(at, CHUNK), slice(None))
        pre = side[here].astype(F32) + received
        squashed = gate(pre)
        message = pre * squashed
        messages[here] = message.astype(BF16)
        slope = squashed + message * (1.0 - squashed)
        grad = (back[here].astype(F32) * slope).astype(BF16)
        grads[here] = grad
        return grad

    outs = (out_left, out_own, out_right)
    edge_groups(counts, send, flip, near, total, outs, chunk_list, edges)


def enc_backward_kernel(
    counts, flip, recv, left, own, right, slope,
    out_left, out_own, out_right, grads, near, total, *chunk_list,
):
    for place, tiles in enumerate((left, own, right)):
        near[3 * place : 3 * place + 3] = tiles[...]

    def edges(chunk, received):
        k, at, _ = chunk
        here = (k, pl.ds(at, CHUNK), slice(None))
        grad = (received * slope[here].astype(F32)).astype(BF16)
        grads[here] = grad
        return grad

    outs = (out_left, out_own, out_right)
    edge_groups(counts, recv, flip, near, total, outs, chunk_list, edges)


def scatter_slots(counts, index_ref, values, total, chunk_list):
    groups = list_chunks(counts, index_ref.shape[2], *chunk_list)
    total[...] = jnp.zeros(total.shape, F32)

    def body(chunks):
        hots = [scatter_hot(rows_of(index_ref, c), total.shape[0], c[2]) for c in chunks]
        rows = [values[k, pl.ds(at, CHUNK), :] for k, at, _ in chunks]
        total[...] += mm(jnp.concatenate(hots, axis=1), jnp.concatenate(rows, axis=0))

    each_group(groups, chunk_list, body)


def dec_sum_kernel(counts, recv, messages, feat, weight, out, total, *chunk_list):
    scatter_slots(counts, recv, messages, total, chunk_list)
    out[...] = (feat[...].astype(F32) + mm(total[...].astype(BF16), weight[...])).astype(BF16)


def dec_local_kernel(counts, recv, grads, out, total, *chunk_list):
    scatter_slots(counts, recv, grads, total, chunk_list)
    out[...] = total[...].astype(BF16)


def enc_scatter_kernel(
    counts, send, grads, cot, local, dec_weight, enc_weight, out, total, *chunk_list
):
    scatter_slots(counts, send, grads, total, chunk_list)
    back = mm_nt(local[...], dec_weight[...])
    back += mm_nt(total[...].astype(BF16), enc_weight[...])
    out[...] = (cot[...].astype(F32) + back).astype(BF16)


def fold_kernel(own, east, west, kept, to_first, to_second):
    total = own[...].astype(F32) + east[...].astype(F32) + west[...].astype(F32)
    kept[...] = total[0]
    to_first[...] = total[1].astype(BF16)
    to_second[...] = total[2].astype(BF16)


def mesh_new_kernel(kept, first, second, feat, out_weight, weight, proj):
    summed = kept[...] + first[...].astype(F32) + second[...].astype(F32)
    update = mm(summed.astype(BF16), out_weight[...])
    proj[...] = mm((feat[...].astype(F32) + update).astype(BF16), weight[...]).astype(BF16)


def mesh_back_kernel(kept, first, second, weight, out_weight, back, enc_back):
    summed = kept[...] + first[...].astype(F32) + second[...].astype(F32)
    exact = mm_nt(summed.astype(BF16), weight[...])
    back[...] = exact
    enc_back[...] = mm_nt(exact.astype(BF16), out_weight[...]).astype(BF16)


def mesh_grad_kernel(kept, first, second, back, weight, out):
    summed = kept[...] + first[...].astype(F32) + second[...].astype(F32)
    out[...] = (back[...] + mm_nt(summed.astype(BF16), weight[...])).astype(BF16)


def along(axis, pairs):
    return lambda value: lax.ppermute(value, axis, pairs)


def lat_pairs(size, start):
    edges = [(i, (i + 1) % size) for i in range(start, size, 2)]
    return edges + [(j, i) for i, j in edges]


def on_device(
    grid_feat, mesh_feat, enc_send, enc_recv, enc_count, dec_send, dec_recv, dec_count,
    enc_src, enc_dst, enc_bias, enc_out, dec_src, dec_dst, dec_bias, dec_out, grid_cot,
):
    grid_rows, width = grid_feat.shape
    mesh_rows = mesh_feat.shape[0]
    cap_e = enc_send.shape[2]
    cap_d = dec_send.shape[2]
    lat_size = lax.axis_size("lat")
    lon_size = lax.axis_size("lon")
    flip = lax.rem(lax.axis_index("lat"), 2).astype(jnp.int32).reshape(1)
    first = along("lat", lat_pairs(lat_size, 0))
    second = along("lat", lat_pairs(lat_size, 1))
    east = along("lon", [(i, (i + 1) % lon_size) for i in range(lon_size)])
    west = along("lon", [((i + 1) % lon_size, i) for i in range(lon_size)])

    def spread(local_tile, name):
        with jax.named_scope(name + "_lat"):
            pieces = [local_tile, first(local_tile), second(local_tile)]
        with jax.named_scope(name + "_lon"):
            three = jnp.stack(pieces)
            return east(three), three, west(three)

    def fold(left, own, right, name):
        with jax.named_scope(name + "_lon"):
            arrived = west(left), east(right)
        kept, to_first, to_second = kernel(
            fold_kernel, [exact_tile, tile, tile], [], name + "_fold", own, *arrived, smem=0
        )
        with jax.named_scope(name + "_lat"):
            return kept, first(to_first), second(to_second)

    def kernel(body, outs, scratch, name, *args, smem=1, mib=12, work=0):
        with jax.named_scope(name):
            return pl.pallas_call(
                body,
                out_shape=outs,
                in_specs=[SMEM] * smem + [VMEM] * (len(args) - smem),
                out_specs=[VMEM] * len(outs),
                scratch_shapes=scratch,
                compiler_params=pltpu.CompilerParams(vmem_limit_bytes=mib * 1024 * 1024),
                cost_estimate=pl.CostEstimate(flops=work, bytes_accessed=0, transcendentals=0),
                name=name,
            )(*args)

    def array(*shape):
        return jax.ShapeDtypeStruct(shape, BF16)

    tile = array(mesh_rows, width)
    exact_tile = jax.ShapeDtypeStruct((mesh_rows, width), F32)
    three = [array(3, mesh_rows, width)] * 3
    enc_slots = [array(9, cap_e, width)]
    dec_slots = [array(9, cap_d, width)]
    grid_tile = [array(grid_rows, width)]
    chunk_list = [pltpu.SMEM((9 * cap_d // CHUNK + GROUP,), jnp.int32)] * 3
    rounded_grid = [pltpu.VMEM((grid_rows, width), BF16)] + chunk_list
    exact_grid = [pltpu.VMEM((grid_rows, width), F32)] + chunk_list
    near = pltpu.VMEM((9, mesh_rows, width), BF16)
    near_split = pltpu.VMEM((9, 2 * mesh_rows, width), BF16)
    near_total = pltpu.VMEM((9, mesh_rows, width), F32)
    enc_work = 2 * grid_rows * width * 9 * cap_e
    dec_work = 2 * grid_rows * width * 9 * cap_d

    enc_send, enc_recv, dec_send, dec_recv = (
        jnp.swapaxes(a, 0, 1) for a in (enc_send, enc_recv, dec_send, dec_recv)
    )

    near_feat = spread(mesh_feat, "e1")
    (sent,) = kernel(
        enc_gather_kernel, enc_slots, rounded_grid, "enc_gather",
        enc_count, enc_send, grid_feat, enc_src, work=enc_work,
    )
    (back_at,) = kernel(
        back_gather_kernel, dec_slots, rounded_grid, "back_gather",
        dec_count, dec_recv, grid_cot, dec_out, work=dec_work,
    )
    (side_at,) = kernel(
        side_gather_kernel, dec_slots, rounded_grid, "side_gather",
        dec_count, dec_recv, grid_feat, dec_dst, dec_bias.reshape(1, width), work=dec_work,
    )

    *enc_partial, slope = kernel(
        enc_forward_kernel, three + enc_slots,
        [near_split, near_total] + chunk_list, "enc_forward",
        enc_count, flip, enc_recv, *near_feat, enc_dst, enc_bias.reshape(1, width), sent,
        smem=2, work=enc_work // 4,
    )
    (dec_proj,) = kernel(
        mesh_new_kernel, [tile], [], "mesh_new",
        *fold(*enc_partial, "f1"), mesh_feat, enc_out, dec_src, smem=0,
    )

    *dec_partial, messages, dec_grads = kernel(
        dec_kernel, three + dec_slots * 2, [near, near_total] + chunk_list, "dec_edges",
        dec_count, flip, dec_send, *spread(dec_proj, "e2"), side_at, back_at,
        smem=2, work=dec_work // 4,
    )
    mesh_back, enc_back = kernel(
        mesh_back_kernel, [exact_tile, tile], [], "mesh_back",
        *fold(*dec_partial, "f2"), dec_src, enc_out, smem=0,
    )

    (grid_new,) = kernel(
        dec_sum_kernel, grid_tile, exact_grid, "dec_sum",
        dec_count, dec_recv, messages, grid_feat, dec_out, work=dec_work,
    )
    (local,) = kernel(
        dec_local_kernel, grid_tile, exact_grid, "dec_local",
        dec_count, dec_recv, dec_grads, work=dec_work,
    )

    *grad_partial, grads = kernel(
        enc_backward_kernel, three + enc_slots, [near, near_total] + chunk_list,
        "enc_backward",
        enc_count, flip, enc_recv, *spread(enc_back, "e3"), slope,
        smem=2, work=enc_work // 4,
    )
    (mesh_grad,) = kernel(
        mesh_grad_kernel, [tile], [], "mesh_grad",
        *fold(*grad_partial, "f3"), mesh_back, enc_dst, smem=0,
    )

    (grid_grad,) = kernel(
        enc_scatter_kernel, grid_tile, exact_grid, "enc_scatter",
        enc_count, enc_send, grads, grid_cot, local, dec_dst, enc_src, work=enc_work,
    )
    return grid_new, mesh_grad, grid_grad


def solution(mesh):
    rows = P(("lat", "lon"), None)
    edges = P(("lat", "lon"), None, None)
    return jax.shard_map(
        on_device,
        mesh=mesh,
        in_specs=(rows, rows, edges, edges, rows, edges, edges, rows)
        + (P(),) * 8
        + (rows,),
        out_specs=(rows, rows, rows),
        check_vma=False,
    )
```

```python
import functools

import jax
import jax.numpy as jnp
from jax import lax
from jax.experimental import pallas as pl
from jax.experimental.pallas import tpu as pltpu
from jax.sharding import PartitionSpec as P


F32 = jnp.float32
BF16 = jnp.bfloat16
LANES = 128
CHUNK = 128
GROUP = 4

VMEM = pl.BlockSpec(memory_space=pltpu.VMEM)
SMEM = pl.BlockSpec(memory_space=pltpu.SMEM)


def mm(lhs, rhs):
    return jnp.dot(lhs, rhs, preferred_element_type=F32)


def mm_nt(lhs, rhs):
    return lax.dot_general(lhs, rhs, (((1,), (1,)), ((), ())), preferred_element_type=F32)


def as_hot(mask):
    return jnp.where(mask, 1.0, 0.0).astype(BF16)


def down_rows(index_row):
    return jnp.transpose(jnp.broadcast_to(index_row, (LANES, index_row.shape[1])))


def gather_hot(index_row, rows):
    spread = down_rows(index_row)
    lane = lax.broadcasted_iota(jnp.int32, spread.shape, 1)
    return jnp.concatenate(
        [as_hot(spread == lane + start) for start in range(0, rows, LANES)], axis=1
    )


def scatter_hot(index_row, rows, live):
    slots = index_row.shape[1]
    slot = lax.broadcasted_iota(jnp.int32, (1, slots), 1)
    index_row = jnp.where(slot < live, index_row, -1)
    return as_hot(lax.broadcasted_iota(jnp.int32, (rows, slots), 0) == index_row)


def gate(pre):
    return 0.5 * jnp.tanh(0.5 * pre) + 0.5


def list_chunks(counts, capacity, block, start, live):
    found = jnp.int32(0)
    for k in range(counts.shape[1]):
        count = counts[0, k]
        for at in range(0, capacity, CHUNK):
            block[found] = k
            start[found] = at
            live[found] = count - at
            found += (count > at).astype(jnp.int32)
    for j in range(GROUP - 1):
        block[found + j] = counts.shape[1] // 2
        start[found + j] = 0
        live[found + j] = 0
    return lax.div(found + (GROUP - 1), GROUP)


def each_group(groups, chunk_list, body):
    block, start, live = chunk_list

    @pl.loop(0, groups)
    def _(g):
        at = [GROUP * g + j for j in range(GROUP)]
        body([(block[n], pl.multiple_of(start[n], CHUNK), live[n]) for n in at])


def rows_of(index_ref, chunk):
    k, at, _ = chunk
    return index_ref[k, :, pl.ds(at, CHUNK)]


def place_of(k, flips):
    def place(offset, flip):
        return jnp.where(offset == 0, 0, jnp.where(offset == 1 - 2 * flip, 1, 2))

    return 3 * place(lax.rem(k, 3) - 1, flips[1]) + place(lax.div(k, 3) - 1, flips[0])


def gather_slots(counts, index_ref, table, out, chunk_list):
    groups = list_chunks(counts, index_ref.shape[2], *chunk_list)

    def body(chunks):
        hots = [gather_hot(rows_of(index_ref, c), table.shape[0]) for c in chunks]
        rows = mm(jnp.concatenate(hots, axis=0), table[...]).astype(BF16)
        for j, (k, at, _) in enumerate(chunks):
            out[k, pl.ds(at, CHUNK), :] = rows[j * CHUNK : (j + 1) * CHUNK]

    each_group(groups, chunk_list, body)


def enc_gather_kernel(counts, send, feat, weight, out, table, *chunk_list):
    table[...] = mm(feat[...], weight[...]).astype(BF16)
    gather_slots(counts, send, table, out, chunk_list)


def side_gather_kernel(cols, counts, recv, feat, weight, bias, out, table, *chunk_list):
    table[...] = (mm(feat[...], weight[:, cols]) + bias[:, cols]).astype(BF16)
    gather_slots(counts, recv, table, out, chunk_list)


def back_gather_kernel(cols, counts, recv, cot, weight, out, table, *chunk_list):
    table[...] = mm_nt(cot[...], weight[cols, :]).astype(BF16)
    gather_slots(counts, recv, table, out, chunk_list)


def near_hot(index_row, rows):
    spread = down_rows(index_row)
    lane = lax.broadcasted_iota(jnp.int32, spread.shape, 1)
    return as_hot(spread == jnp.where(lane < rows, lane, lane - rows))


def edge_groups(counts, index_ref, flips, side, total, outs, chunk_list, edges):
    rows = total.shape[1]
    groups = list_chunks(counts, index_ref.shape[2], *chunk_list)
    total[...] = jnp.zeros(total.shape, F32)

    def body(chunks):
        places = [place_of(k, flips) for k, _, _ in chunks]
        index_rows = [rows_of(index_ref, chunk) for chunk in chunks]

        def gather(j):
            return mm(near_hot(index_rows[j], rows)[:, : side.shape[1]], side[places[j]])

        received = gather(0)
        for j, chunk in enumerate(chunks):
            following = gather(j + 1) if j + 1 < len(chunks) else None
            value = edges(chunk, received)
            total[places[j]] += mm(scatter_hot(index_rows[j], rows, chunk[2]), value)
            received = following

    each_group(groups, chunk_list, body)
    for place, out in enumerate(outs):
        out[...] = total[3 * place : 3 * place + 3].astype(BF16)


def enc_forward_kernel(
    counts, flips, recv, own, first, second, weight, bias, sent,
    out_own, out_first, out_second, slope, side, total, *chunk_list,
):
    rows = own.shape[1]
    for place, near in enumerate((own, first, second)):
        feats = near[...].reshape(3 * rows, near.shape[2])
        exact = mm(feats, weight[...]) + bias[...]
        high = exact.astype(BF16)
        low = (exact - high.astype(F32)).astype(BF16)
        side[3 * place : 3 * place + 3, :rows, :] = high.reshape(3, rows, -1)
        side[3 * place : 3 * place + 3, rows:, :] = low.reshape(3, rows, -1)

    def edges(chunk, received):
        k, at, _ = chunk
        pre = sent[k, pl.ds(at, CHUNK), :].astype(F32) + received
        squashed = gate(pre)
        message = pre * squashed
        slope[k, pl.ds(at, CHUNK), :] = (squashed + message * (1.0 - squashed)).astype(BF16)
        return message.astype(BF16)

    outs = (out_own, out_first, out_second)
    edge_groups(counts, recv, flips, side, total, outs, chunk_list, edges)


def halves(lower, upper, at):
    return jnp.concatenate([lower[at], upper[at]], axis=1).astype(F32)


def dec_kernel(
    counts, flips, send, own, first, second, side_a, side_b, back_a, back_b,
    out_own, out_first, out_second, messages, grads, near, total, *chunk_list,
):
    for place, tiles in enumerate((own, first, second)):
        near[3 * place : 3 * place + 3] = tiles[...]

    def edges(chunk, received):
        k, at, _ = chunk
        here = (k, pl.ds(at, CHUNK), slice(None))
        pre = halves(side_a, side_b, here) + received
        squashed = gate(pre)
        message = pre * squashed
        messages[here] = message.astype(BF16)
        slope = squashed + message * (1.0 - squashed)
        grad = (halves(back_a, back_b, here) * slope).astype(BF16)
        grads[here] = grad
        return grad

    outs = (out_own, out_first, out_second)
    edge_groups(counts, send, flips, near, total, outs, chunk_list, edges)


def enc_backward_kernel(
    counts, flips, recv, own, first, second, slope,
    out_own, out_first, out_second, grads, near, total, *chunk_list,
):
    for place, tiles in enumerate((own, first, second)):
        near[3 * place : 3 * place + 3] = tiles[...]

    def edges(chunk, received):
        k, at, _ = chunk
        here = (k, pl.ds(at, CHUNK), slice(None))
        grad = (received * slope[here].astype(F32)).astype(BF16)
        grads[here] = grad
        return grad

    outs = (out_own, out_first, out_second)
    edge_groups(counts, recv, flips, near, total, outs, chunk_list, edges)


def scatter_slots(counts, index_ref, values, total, chunk_list, cols=slice(None)):
    groups = list_chunks(counts, index_ref.shape[2], *chunk_list)
    total[...] = jnp.zeros(total.shape, F32)

    def body(chunks):
        hots = [scatter_hot(rows_of(index_ref, c), total.shape[0], c[2]) for c in chunks]
        rows = [values[k, pl.ds(at, CHUNK), cols] for k, at, _ in chunks]
        total[...] += mm(jnp.concatenate(hots, axis=1), jnp.concatenate(rows, axis=0))

    each_group(groups, chunk_list, body)


def scatter_kernel(cols, counts, index_ref, values, out, total, *chunk_list):
    scatter_slots(counts, index_ref, values, total, chunk_list, cols)
    out[...] = total[...].astype(BF16)


def grid_new_kernel(
    cols, counts, recv, messages, feat, lower, weight, out, total, *chunk_list
):
    scatter_slots(counts, recv, messages, total, chunk_list, cols)
    half = lower.shape[1]
    update = mm(lower[...], weight[:half, :]) + mm(total[...].astype(BF16), weight[half:, :])
    out[...] = (feat[...].astype(F32) + update).astype(BF16)


def grid_grad_kernel(
    cols, counts, send, grads, cot, dec_lower, dec_upper, lower, dec_weight, enc_weight,
    out, total, *chunk_list,
):
    scatter_slots(counts, send, grads, total, chunk_list, cols)
    half = lower.shape[1]
    back = mm_nt(dec_lower[...], dec_weight[:, :half]) + mm_nt(dec_upper[...], dec_weight[:, half:])
    back += mm_nt(lower[...], enc_weight[:, :half])
    back += mm_nt(total[...].astype(BF16), enc_weight[:, half:])
    out[...] = (cot[...].astype(F32) + back).astype(BF16)


def fold_kernel(own, east, west, kept, to_first, to_second):
    total = own[...].astype(F32) + east[...].astype(F32) + west[...].astype(F32)
    kept[...] = total[0]
    to_first[...] = total[1].astype(BF16)
    to_second[...] = total[2].astype(BF16)


def mesh_new_kernel(kept, first, second, feat, out_weight, weight, proj):
    summed = kept[...] + first[...].astype(F32) + second[...].astype(F32)
    update = mm(summed.astype(BF16), out_weight[...])
    proj[...] = mm((feat[...].astype(F32) + update).astype(BF16), weight[...]).astype(BF16)


def mesh_back_kernel(kept, first, second, weight, out_weight, back, enc_back):
    summed = kept[...] + first[...].astype(F32) + second[...].astype(F32)
    exact = mm_nt(summed.astype(BF16), weight[...])
    back[...] = exact
    enc_back[...] = mm_nt(exact.astype(BF16), out_weight[...]).astype(BF16)


def mesh_grad_kernel(kept, first, second, back, weight, out):
    summed = kept[...] + first[...].astype(F32) + second[...].astype(F32)
    out[...] = (back[...] + mm_nt(summed.astype(BF16), weight[...])).astype(BF16)


def along(axis, pairs):
    return lambda value: lax.ppermute(value, axis, pairs)


def swaps(size, start):
    edges = [(i, (i + 1) % size) for i in range(start, size, 2)]
    return edges + [(j, i) for i, j in edges]


def on_device(
    grid_feat, mesh_feat, enc_send, enc_recv, enc_count, dec_send, dec_recv, dec_count,
    enc_src, enc_dst, enc_bias, enc_out, dec_src, dec_dst, dec_bias, dec_out, grid_cot,
):
    grid_rows, width = grid_feat.shape
    mesh_rows = mesh_feat.shape[0]
    cap_e = enc_send.shape[2]
    cap_d = dec_send.shape[2]
    lat_size = lax.axis_size("lat")
    lon_size = lax.axis_size("lon")
    flips = jnp.stack([lax.rem(lax.axis_index(a), 2) for a in ("lat", "lon")]).astype(jnp.int32)
    lat_first, lat_second = (along("lat", swaps(lat_size, i)) for i in range(2))
    lon_first, lon_second = (along("lon", swaps(lon_size, i)) for i in range(2))

    def spread(local_tile):
        pieces = [local_tile, lat_first(local_tile), lat_second(local_tile)]
        three = jnp.stack(pieces)
        return three, lon_first(three), lon_second(three)

    def fold(own, to_first, to_second):
        arrived = lon_first(to_first), lon_second(to_second)
        kept, to_first, to_second = kernel(
            fold_kernel, [exact_tile, tile, tile], [], own, *arrived, smem=0
        )
        return kept, lat_first(to_first), lat_second(to_second)

    def kernel(body, outs, scratch, *args, smem=1, mib=12, work=0):
        return pl.pallas_call(
            body,
            out_shape=outs,
            in_specs=[SMEM] * smem + [VMEM] * (len(args) - smem),
            out_specs=[VMEM] * len(outs),
            scratch_shapes=scratch,
            compiler_params=pltpu.CompilerParams(vmem_limit_bytes=mib * 1024 * 1024),
            cost_estimate=pl.CostEstimate(flops=work, bytes_accessed=0, transcendentals=0),
        )(*args)

    def array(*shape):
        return jax.ShapeDtypeStruct(shape, BF16)

    tile = array(mesh_rows, width)
    exact_tile = jax.ShapeDtypeStruct((mesh_rows, width), F32)
    three = [array(3, mesh_rows, width)] * 3
    enc_slots = [array(9, cap_e, width)]
    dec_slots = [array(9, cap_d, width)]
    grid_tile = [array(grid_rows, width)]
    chunk_list = [pltpu.SMEM((9 * cap_d // CHUNK + GROUP,), jnp.int32)] * 3
    lower, upper = slice(0, width // 2), slice(width // 2, width)
    half_grid = [array(grid_rows, width // 2)]
    half_slots = [array(9, cap_d, width // 2)]
    rounded_half = [pltpu.VMEM((grid_rows, width // 2), BF16)] + chunk_list
    exact_half = [pltpu.VMEM((grid_rows, width // 2), F32)] + chunk_list
    rounded_grid = [pltpu.VMEM((grid_rows, width), BF16)] + chunk_list
    near = pltpu.VMEM((9, mesh_rows, width), BF16)
    near_split = pltpu.VMEM((9, 2 * mesh_rows, width), BF16)
    near_total = pltpu.VMEM((9, mesh_rows, width), F32)
    enc_work = 2 * grid_rows * width * 9 * cap_e
    dec_work = 2 * grid_rows * width * 9 * cap_d

    enc_send, enc_recv, dec_send, dec_recv = (
        jnp.swapaxes(a, 0, 1) for a in (enc_send, enc_recv, dec_send, dec_recv)
    )

    near_feat = spread(mesh_feat)
    (sent,) = kernel(
        enc_gather_kernel, enc_slots, rounded_grid,
        enc_count, enc_send, grid_feat, enc_src, work=enc_work,
    )
    back_at = [
        kernel(
            functools.partial(back_gather_kernel, cols), half_slots, rounded_half,
            dec_count, dec_recv, grid_cot, dec_out, work=dec_work // 2,
        )[0]
        for cols in (lower, upper)
    ]
    side_at = [
        kernel(
            functools.partial(side_gather_kernel, cols), half_slots, rounded_half,
            dec_count, dec_recv, grid_feat, dec_dst, dec_bias.reshape(1, width),
            work=dec_work // 2,
        )[0]
        for cols in (lower, upper)
    ]

    *enc_partial, slope = kernel(
        enc_forward_kernel, three + enc_slots,
        [near_split, near_total] + chunk_list,
        enc_count, flips, enc_recv, *near_feat, enc_dst, enc_bias.reshape(1, width), sent,
        smem=2, work=enc_work // 4,
    )
    (dec_proj,) = kernel(
        mesh_new_kernel, [tile], [],
        *fold(*enc_partial), mesh_feat, enc_out, dec_src, smem=0,
    )

    *dec_partial, messages, dec_grads = kernel(
        dec_kernel, three + dec_slots * 2, [near, near_total] + chunk_list,
        dec_count, flips, dec_send, *spread(dec_proj), *side_at, *back_at,
        smem=2, work=dec_work // 4,
    )
    mesh_back, enc_back = kernel(
        mesh_back_kernel, [exact_tile, tile], [],
        *fold(*dec_partial), dec_src, enc_out, smem=0,
    )

    (sum_lower,) = kernel(
        functools.partial(scatter_kernel, lower), half_grid, exact_half,
        dec_count, dec_recv, messages, work=dec_work // 2,
    )
    (grid_new,) = kernel(
        functools.partial(grid_new_kernel, upper), grid_tile, exact_half,
        dec_count, dec_recv, messages, grid_feat, sum_lower, dec_out, work=dec_work // 2,
    )
    dec_local = [
        kernel(
            functools.partial(scatter_kernel, cols), half_grid, exact_half,
            dec_count, dec_recv, dec_grads, work=dec_work // 2,
        )[0]
        for cols in (lower, upper)
    ]

    *grad_partial, grads = kernel(
        enc_backward_kernel, three + enc_slots, [near, near_total] + chunk_list,
        enc_count, flips, enc_recv, *spread(enc_back), slope,
        smem=2, work=enc_work // 4,
    )
    (mesh_grad,) = kernel(
        mesh_grad_kernel, [tile], [],
        *fold(*grad_partial), mesh_back, enc_dst, smem=0,
    )

    (total_lower,) = kernel(
        functools.partial(scatter_kernel, lower), half_grid, exact_half,
        enc_count, enc_send, grads, work=enc_work // 2,
    )
    (grid_grad,) = kernel(
        functools.partial(grid_grad_kernel, upper), grid_tile, exact_half,
        enc_count, enc_send, grads, grid_cot, *dec_local, total_lower, dec_dst, enc_src,
        work=enc_work // 2,
    )
    return grid_new, mesh_grad, grid_grad


def solution(mesh):
    rows = P(("lat", "lon"), None)
    edges = P(("lat", "lon"), None, None)
    return jax.shard_map(
        on_device,
        mesh=mesh,
        in_specs=(rows, rows, edges, edges, rows, edges, edges, rows)
        + (P(),) * 8
        + (rows,),
        out_specs=(rows, rows, rows),
        check_vma=False,
    )
```

```python
import functools

import jax
import jax.numpy as jnp
from jax import lax
from jax.experimental import pallas as pl
from jax.experimental.pallas import tpu as pltpu
from jax.sharding import PartitionSpec as P


F32 = jnp.float32
BF16 = jnp.bfloat16
LANES = 128
CHUNK = 128
GROUP = 4

ANY = pl.BlockSpec(memory_space=pl.ANY)
VMEM = pl.BlockSpec(memory_space=pltpu.VMEM)
SMEM = pl.BlockSpec(memory_space=pltpu.SMEM)


def mm(lhs, rhs):
    return jnp.dot(lhs, rhs, preferred_element_type=F32)


def mm_nt(lhs, rhs):
    return lax.dot_general(lhs, rhs, (((1,), (1,)), ((), ())), preferred_element_type=F32)


def as_hot(mask):
    return jnp.where(mask, 1.0, 0.0).astype(BF16)


def down_rows(index_row):
    return jnp.transpose(jnp.broadcast_to(index_row, (LANES, index_row.shape[1])))


def gather_hot(index_row, rows):
    spread = down_rows(index_row)
    lane = lax.broadcasted_iota(jnp.int32, spread.shape, 1)
    return jnp.concatenate(
        [as_hot(spread == lane + start) for start in range(0, rows, LANES)], axis=1
    )


def scatter_hot(index_row, rows, live):
    slots = index_row.shape[1]
    slot = lax.broadcasted_iota(jnp.int32, (1, slots), 1)
    index_row = jnp.where(slot < live, index_row, -1)
    return as_hot(lax.broadcasted_iota(jnp.int32, (rows, slots), 0) == index_row)


def gate(pre):
    return 0.5 * jnp.tanh(0.5 * pre) + 0.5


def list_chunks(counts, capacity, block, start, live, blocks=range(9)):
    found = jnp.int32(0)
    for k in blocks:
        count = counts[0, k]
        for at in range(0, capacity, CHUNK):
            block[found] = k
            start[found] = at
            live[found] = count - at
            found += (count > at).astype(jnp.int32)
    last = jnp.maximum(found - 1, 0)
    for j in range(GROUP - 1):
        block[found + j] = block[last]
        start[found + j] = start[last]
        live[found + j] = 0
    return lax.div(found + (GROUP - 1), GROUP)


def each_group(groups, chunk_list, body):
    block, start, live = chunk_list

    @pl.loop(0, groups)
    def _(g):
        at = [GROUP * g + j for j in range(GROUP)]
        body([(block[n], pl.multiple_of(start[n], CHUNK), live[n]) for n in at])


def rows_of(index_ref, chunk):
    k, at, _ = chunk
    return index_ref[k, :, pl.ds(at, CHUNK)]


def place_of(k, flips):
    def place(offset, flip):
        return jnp.where(offset == 0, 0, jnp.where(offset == 1 - 2 * flip, 1, 2))

    return 3 * place(lax.rem(k, 3) - 1, flips[1]) + place(lax.div(k, 3) - 1, flips[0])


def gather_slots(counts, index_ref, table, out, chunk_list):
    groups = list_chunks(counts, index_ref.shape[2], *chunk_list)

    def body(chunks):
        hots = [gather_hot(rows_of(index_ref, c), table.shape[0]) for c in chunks]
        rows = mm(jnp.concatenate(hots, axis=0), table[...]).astype(BF16)
        for j, (k, at, _) in enumerate(chunks):
            out[k, pl.ds(at, CHUNK), :] = rows[j * CHUNK : (j + 1) * CHUNK]

    each_group(groups, chunk_list, body)


def enc_gather_kernel(
    counts, send, feat, weight, out, table, send_in, feat_in, weight_in, sems, *chunk_list
):
    pairs = ((feat, feat_in), (weight, weight_in), (send, send_in))
    copies = [pltpu.make_async_copy(a, b, sems.at[i]) for i, (a, b) in enumerate(pairs)]
    for copy in copies:
        copy.start()
    for copy in copies:
        copy.wait()
    table[...] = mm(feat_in[...], weight_in[...]).astype(BF16)
    gather_slots(counts, send_in, table, out, chunk_list)


def side_gather_kernel(cols, counts, recv, feat, weight, bias, out, table, *chunk_list):
    table[...] = (mm(feat[...], weight[:, cols]) + bias[:, cols]).astype(BF16)
    gather_slots(counts, recv, table, out, chunk_list)


def back_gather_kernel(cols, counts, recv, cot, weight, out, table, *chunk_list):
    table[...] = mm_nt(cot[...], weight[cols, :]).astype(BF16)
    gather_slots(counts, recv, table, out, chunk_list)


def near_hot(index_row, rows):
    spread = down_rows(index_row)
    lane = lax.broadcasted_iota(jnp.int32, spread.shape, 1)
    return as_hot(spread == jnp.where(lane < rows, lane, lane - rows))


def edge_groups(counts, index_ref, flips, side, total, outs, chunk_list, edges):
    rows = total.shape[1]
    ours = len(outs) == 1
    blocks = [k for k in range(9) if (k % 3 == 1) == ours]
    groups = list_chunks(counts, index_ref.shape[2], *chunk_list, blocks=blocks)
    total[...] = jnp.zeros(total.shape, F32)

    def body(chunks):
        places = [place_of(k, flips) - (0 if ours else 3) for k, _, _ in chunks]
        index_rows = [rows_of(index_ref, chunk) for chunk in chunks]

        def gather(j):
            return mm(near_hot(index_rows[j], rows)[:, : side.shape[1]], side[places[j]])

        received = gather(0)
        for j, chunk in enumerate(chunks):
            following = gather(j + 1) if j + 1 < len(chunks) else None
            value = edges(chunk, received)
            total[places[j]] += mm(scatter_hot(index_rows[j], rows, chunk[2]), value)
            received = following

    each_group(groups, chunk_list, body)
    for place, out in enumerate(outs):
        out[...] = total[3 * place : 3 * place + 3].astype(BF16)


def stack_near(nears, side):
    for place, tiles in enumerate(nears):
        side[3 * place : 3 * place + 3] = tiles[...]


def enc_forward_kernel(n, counts, flips, recv, *refs):
    nears, (weight, bias, sent), refs = refs[:n], refs[n : n + 3], refs[n + 3 + (n == 1) :]
    outs, (slope, side, total, *chunk_list) = refs[:n], refs[n:]
    rows = total.shape[1]
    for place, near in enumerate(nears):
        feats = near[...].reshape(3 * rows, near.shape[2])
        exact = mm(feats, weight[...]) + bias[...]
        high = exact.astype(BF16)
        low = (exact - high.astype(F32)).astype(BF16)
        side[3 * place : 3 * place + 3, :rows, :] = high.reshape(3, rows, -1)
        side[3 * place : 3 * place + 3, rows:, :] = low.reshape(3, rows, -1)

    def edges(chunk, received):
        k, at, _ = chunk
        pre = sent[k, pl.ds(at, CHUNK), :].astype(F32) + received
        squashed = gate(pre)
        message = pre * squashed
        slope[k, pl.ds(at, CHUNK), :] = (squashed + message * (1.0 - squashed)).astype(BF16)
        return message.astype(BF16)

    edge_groups(counts, recv, flips, side, total, outs, chunk_list, edges)


def halves(lower, upper, at):
    return jnp.concatenate([lower[at], upper[at]], axis=1).astype(F32)


def dec_kernel(n, counts, flips, send, *refs):
    nears, tables, refs = refs[:n], refs[n : n + 4], refs[n + 4 + 2 * (n == 1) :]
    outs, (messages, grads, near, total, *chunk_list) = refs[:n], refs[n:]
    stack_near(nears, near)

    def edges(chunk, received):
        k, at, _ = chunk
        here = (k, pl.ds(at, CHUNK), slice(None))
        pre = halves(*tables[:2], here) + received
        squashed = gate(pre)
        message = pre * squashed
        messages[here] = message.astype(BF16)
        slope = squashed + message * (1.0 - squashed)
        grad = (halves(*tables[2:], here) * slope).astype(BF16)
        grads[here] = grad
        return grad

    edge_groups(counts, send, flips, near, total, outs, chunk_list, edges)


def enc_backward_kernel(n, counts, flips, recv, *refs):
    nears, slope, refs = refs[:n], refs[n], refs[n + 1 + (n == 1) :]
    outs, (grads, near, total, *chunk_list) = refs[:n], refs[n:]
    stack_near(nears, near)

    def edges(chunk, received):
        k, at, _ = chunk
        here = (k, pl.ds(at, CHUNK), slice(None))
        grad = (received * slope[here].astype(F32)).astype(BF16)
        grads[here] = grad
        return grad

    edge_groups(counts, recv, flips, near, total, outs, chunk_list, edges)


def scatter_slots(counts, index_ref, values, total, chunk_list, cols=slice(None)):
    groups = list_chunks(counts, index_ref.shape[2], *chunk_list)
    total[...] = jnp.zeros(total.shape, F32)

    def body(chunks):
        hots = [scatter_hot(rows_of(index_ref, c), total.shape[0], c[2]) for c in chunks]
        rows = [values[k, pl.ds(at, CHUNK), cols] for k, at, _ in chunks]
        total[...] += mm(jnp.concatenate(hots, axis=1), jnp.concatenate(rows, axis=0))

    each_group(groups, chunk_list, body)


def scatter_kernel(cols, counts, index_ref, values, out, total, *chunk_list):
    scatter_slots(counts, index_ref, values, total, chunk_list, cols)
    out[...] = total[...].astype(BF16)


def grid_new_kernel(
    cols, counts, recv, messages, feat, lower, weight, out, total, *chunk_list
):
    scatter_slots(counts, recv, messages, total, chunk_list, cols)
    half = lower.shape[1]
    update = mm(lower[...], weight[:half, :]) + mm(total[...].astype(BF16), weight[half:, :])
    out[...] = (feat[...].astype(F32) + update).astype(BF16)


def dec_grid_kernel(
    cols, counts, recv, grads, cot, lower, weight, out, total, *chunk_list
):
    scatter_slots(counts, recv, grads, total, chunk_list, cols)
    half = lower.shape[1]
    back = mm_nt(lower[...], weight[:, :half])
    back += mm_nt(total[...].astype(BF16), weight[:, half:])
    out[...] = cot[...].astype(F32) + back


def grid_grad_kernel(counts, send, grads, partial, weight, out, total, *chunk_list):
    scatter_slots(counts, send, grads, total, chunk_list)
    back = mm_nt(total[...].astype(BF16), weight[...])
    out[...] = (partial[...] + back).astype(BF16)


def fold_kernel(own, east, west, kept, to_first, to_second):
    total = own[...].astype(F32) + east[...].astype(F32) + west[...].astype(F32)
    kept[...] = total[0]
    to_first[...] = total[1].astype(BF16)
    to_second[...] = total[2].astype(BF16)


def mesh_new_kernel(kept, first, second, feat, out_weight, weight, proj):
    summed = kept[...] + first[...].astype(F32) + second[...].astype(F32)
    update = mm(summed.astype(BF16), out_weight[...])
    proj[...] = mm((feat[...].astype(F32) + update).astype(BF16), weight[...]).astype(BF16)


def mesh_back_kernel(kept, first, second, weight, out_weight, back, enc_back):
    summed = kept[...] + first[...].astype(F32) + second[...].astype(F32)
    exact = mm_nt(summed.astype(BF16), weight[...])
    back[...] = exact
    enc_back[...] = mm_nt(exact.astype(BF16), out_weight[...]).astype(BF16)


def mesh_grad_kernel(kept, first, second, back, weight, out):
    summed = kept[...] + first[...].astype(F32) + second[...].astype(F32)
    out[...] = (back[...] + mm_nt(summed.astype(BF16), weight[...])).astype(BF16)


def along(axis, pairs):
    return lambda value: lax.ppermute(value, axis, pairs)


def swaps(size, start):
    edges = [(i, (i + 1) % size) for i in range(start, size, 2)]
    return edges + [(j, i) for i, j in edges]


def on_device(
    grid_feat, mesh_feat, enc_send, enc_recv, enc_count, dec_send, dec_recv, dec_count,
    enc_src, enc_dst, enc_bias, enc_out, dec_src, dec_dst, dec_bias, dec_out, grid_cot,
):
    grid_rows, width = grid_feat.shape
    mesh_rows = mesh_feat.shape[0]
    cap_e = enc_send.shape[2]
    cap_d = dec_send.shape[2]
    lat_size = lax.axis_size("lat")
    lon_size = lax.axis_size("lon")
    flips = jnp.stack([lax.rem(lax.axis_index(a), 2) for a in ("lat", "lon")]).astype(jnp.int32)
    lat_first, lat_second = (along("lat", swaps(lat_size, i)) for i in range(2))
    lon_first, lon_second = (along("lon", swaps(lon_size, i)) for i in range(2))

    def spread(local_tile):
        pieces = [local_tile, lat_first(local_tile), lat_second(local_tile)]
        three = jnp.stack(pieces)
        return three, lon_first(three), lon_second(three)

    def fold(own, to_first, to_second):
        arrived = lon_first(to_first), lon_second(to_second)
        kept, to_first, to_second = kernel(
            fold_kernel, [exact_tile, tile, tile], [], own, *arrived, smem=0
        )
        return kept, lat_first(to_first), lat_second(to_second)

    def kernel(body, outs, scratch, *args, smem=1, mib=12, work=0, specs=None, alias=()):
        return pl.pallas_call(
            body,
            out_shape=outs,
            in_specs=specs or [SMEM] * smem + [VMEM] * (len(args) - smem),
            input_output_aliases=dict(alias),
            out_specs=[VMEM] * len(outs),
            scratch_shapes=scratch,
            compiler_params=pltpu.CompilerParams(vmem_limit_bytes=mib * 1024 * 1024),
            cost_estimate=pl.CostEstimate(flops=work, bytes_accessed=0, transcendentals=0),
        )(*args)

    def array(*shape):
        return jax.ShapeDtypeStruct(shape, BF16)

    tile = array(mesh_rows, width)
    exact_tile = jax.ShapeDtypeStruct((mesh_rows, width), F32)
    three = [array(3, mesh_rows, width)] * 3
    enc_slots = [array(9, cap_e, width)]
    dec_slots = [array(9, cap_d, width)]
    grid_tile = [array(grid_rows, width)]
    chunk_list = [pltpu.SMEM((9 * cap_d // CHUNK + GROUP,), jnp.int32)] * 3
    lower, upper = slice(0, width // 2), slice(width // 2, width)
    half_grid = [array(grid_rows, width // 2)]
    half_slots = [array(9, cap_d, width // 2)]
    rounded_half = [pltpu.VMEM((grid_rows, width // 2), BF16)] + chunk_list
    exact_half = [pltpu.VMEM((grid_rows, width // 2), F32)] + chunk_list
    rounded_grid = [pltpu.VMEM((grid_rows, width), BF16)] + chunk_list
    near = (mesh_rows, width), BF16
    near_split = (2 * mesh_rows, width), BF16
    near_total = (mesh_rows, width), F32
    enc_work = 2 * grid_rows * width * 9 * cap_e
    dec_work = 2 * grid_rows * width * 9 * cap_d

    enc_send, enc_recv, dec_send, dec_recv = (
        jnp.swapaxes(a, 0, 1) for a in (enc_send, enc_recv, dec_send, dec_recv)
    )

    near_feat = spread(mesh_feat)
    (sent,) = kernel(
        enc_gather_kernel, enc_slots,
        [
            rounded_grid[0],
            pltpu.VMEM((9, 1, cap_e), jnp.int32),
            pltpu.VMEM((grid_rows, width), BF16),
            pltpu.VMEM((width, width), BF16),
            pltpu.SemaphoreType.DMA((3,)),
            *chunk_list,
        ],
        enc_count, enc_send, grid_feat, enc_src,
        work=enc_work, specs=[SMEM, ANY, ANY, ANY],
    )
    back_at = [
        kernel(
            functools.partial(back_gather_kernel, cols), half_slots, rounded_half,
            dec_count, dec_recv, grid_cot, dec_out, work=dec_work // 2,
        )[0]
        for cols in (lower, upper)
    ]
    side_at = [
        kernel(
            functools.partial(side_gather_kernel, cols), half_slots, rounded_half,
            dec_count, dec_recv, grid_feat, dec_dst, dec_bias.reshape(1, width),
            work=dec_work // 2,
        )[0]
        for cols in (lower, upper)
    ]

    def edges(body, counts, index, nears, extra, slots, scratch, work):
        outs = []
        fill = []
        for n in (2, 1):
            args = (counts, flips, index, *(nears[1:] if n == 2 else nears[:1]), *extra, *fill)
            base = len(args) - len(fill)
            made = kernel(
                functools.partial(body, n), three[:n] + slots,
                [pltpu.VMEM((3 * n,) + shape, kind) for shape, kind in scratch] + chunk_list,
                *args, smem=2, work=n * work // 3,
                alias=[(base + i, n + i) for i in range(len(fill))],
            )
            outs = list(made[:n]) + outs
            fill = made[n:]
        return outs, fill

    enc_partial, (slope,) = edges(
        enc_forward_kernel, enc_count, enc_recv, near_feat,
        (enc_dst, enc_bias.reshape(1, width), sent), enc_slots, [near_split, near_total],
        enc_work // 4,
    )
    (dec_proj,) = kernel(
        mesh_new_kernel, [tile], [],
        *fold(*enc_partial), mesh_feat, enc_out, dec_src, smem=0,
    )

    dec_partial, (messages, dec_grads) = edges(
        dec_kernel, dec_count, dec_send, spread(dec_proj),
        (*side_at, *back_at), dec_slots * 2, [near, near_total], dec_work // 4,
    )
    mesh_back, enc_back = kernel(
        mesh_back_kernel, [exact_tile, tile], [],
        *fold(*dec_partial), dec_src, enc_out, smem=0,
    )

    (sum_lower,) = kernel(
        functools.partial(scatter_kernel, lower), half_grid, exact_half,
        dec_count, dec_recv, messages, work=dec_work // 2,
    )
    (grid_new,) = kernel(
        functools.partial(grid_new_kernel, upper), grid_tile, exact_half,
        dec_count, dec_recv, messages, grid_feat, sum_lower, dec_out, work=dec_work // 2,
    )
    (local_lower,) = kernel(
        functools.partial(scatter_kernel, lower), half_grid, exact_half,
        dec_count, dec_recv, dec_grads, work=dec_work // 2,
    )
    (dec_grid,) = kernel(
        functools.partial(dec_grid_kernel, upper),
        [jax.ShapeDtypeStruct((grid_rows, width), F32)], exact_half,
        dec_count, dec_recv, dec_grads, grid_cot, local_lower, dec_dst, work=dec_work // 2,
    )

    grad_partial, (grads,) = edges(
        enc_backward_kernel, enc_count, enc_recv, spread(enc_back),
        (slope,), enc_slots, [near, near_total], enc_work // 4,
    )
    (mesh_grad,) = kernel(
        mesh_grad_kernel, [tile], [],
        *fold(*grad_partial), mesh_back, enc_dst, smem=0,
    )

    (grid_grad,) = kernel(
        grid_grad_kernel, grid_tile,
        [pltpu.VMEM((grid_rows, width), F32)] + chunk_list,
        enc_count, enc_send, grads, dec_grid, enc_src, work=enc_work,
    )
    return grid_new, mesh_grad, grid_grad


def solution(mesh):
    rows = P(("lat", "lon"), None)
    edges = P(("lat", "lon"), None, None)
    return jax.shard_map(
        on_device,
        mesh=mesh,
        in_specs=(rows, rows, edges, edges, rows, edges, edges, rows)
        + (P(),) * 8
        + (rows,),
        out_specs=(rows, rows, rows),
        check_vma=False,
    )
```

```python
import functools

import jax
import jax.numpy as jnp
from jax import lax
from jax.experimental import pallas as pl
from jax.experimental.pallas import tpu as pltpu
from jax.sharding import PartitionSpec as P


F32 = jnp.float32
BF16 = jnp.bfloat16
LANES = 128
CHUNK = 128
GROUP = 4

HBM = pl.BlockSpec(memory_space=pltpu.HBM)
VMEM = pl.BlockSpec(memory_space=pltpu.VMEM)
SMEM = pl.BlockSpec(memory_space=pltpu.SMEM)


def mm(lhs, rhs):
    return jnp.dot(lhs, rhs, preferred_element_type=F32)


def mm_nt(lhs, rhs):
    return lax.dot_general(lhs, rhs, (((1,), (1,)), ((), ())), preferred_element_type=F32)


def as_hot(mask):
    return jnp.where(mask, 1.0, 0.0).astype(BF16)


def down_rows(index_row):
    return jnp.transpose(jnp.broadcast_to(index_row, (LANES, index_row.shape[1])))


def gather_hot(index_row, rows):
    spread = down_rows(index_row)
    lane = lax.broadcasted_iota(jnp.int32, spread.shape, 1)
    return jnp.concatenate(
        [as_hot(spread == lane + start) for start in range(0, rows, LANES)], axis=1
    )


def scatter_hot(index_row, rows, live):
    slots = index_row.shape[1]
    slot = lax.broadcasted_iota(jnp.int32, (1, slots), 1)
    index_row = jnp.where(slot < live, index_row, -1)
    return as_hot(lax.broadcasted_iota(jnp.int32, (rows, slots), 0) == index_row)


def gate(pre):
    return 0.5 * jnp.tanh(0.5 * pre) + 0.5


def list_chunks(counts, capacity, block, start, live, blocks=range(9)):
    found = jnp.int32(0)
    for k in blocks:
        count = counts[0, k]
        for at in range(0, capacity, CHUNK):
            block[found] = k
            start[found] = at
            live[found] = count - at
            found += (count > at).astype(jnp.int32)
    last = jnp.maximum(found - 1, 0)
    for j in range(GROUP - 1):
        block[found + j] = block[last]
        start[found + j] = start[last]
        live[found + j] = 0
    return lax.div(found + (GROUP - 1), GROUP)


def each_group(groups, chunk_list, body):
    block, start, live = chunk_list

    @pl.loop(0, groups)
    def _(g):
        at = [GROUP * g + j for j in range(GROUP)]
        body([(block[n], pl.multiple_of(start[n], CHUNK), live[n]) for n in at])


def rows_of(index_ref, chunk):
    k, at, _ = chunk
    return index_ref[k, :, pl.ds(at, CHUNK)]


def place_of(k, flips):
    def place(offset, flip):
        return jnp.where(offset == 0, 0, jnp.where(offset == 1 - 2 * flip, 1, 2))

    return 3 * place(lax.rem(k, 3) - 1, flips[1]) + place(lax.div(k, 3) - 1, flips[0])


def gather_slots(counts, index_ref, table, out, chunk_list):
    groups = list_chunks(counts, index_ref.shape[2], *chunk_list)

    def body(chunks):
        hots = [gather_hot(rows_of(index_ref, c), table.shape[0]) for c in chunks]
        rows = mm(jnp.concatenate(hots, axis=0), table[...]).astype(BF16)
        for j, (k, at, _) in enumerate(chunks):
            out[k, pl.ds(at, CHUNK), :] = rows[j * CHUNK : (j + 1) * CHUNK]

    each_group(groups, chunk_list, body)


def enc_gather_kernel(
    counts, send, feat, weight, out, table, send_in, feat_in, weight_in, sems, *chunk_list
):
    pairs = ((feat, feat_in), (weight, weight_in), (send, send_in))
    copies = [pltpu.make_async_copy(a, b, sems.at[i]) for i, (a, b) in enumerate(pairs)]
    for copy in copies:
        copy.start()
    for copy in copies:
        copy.wait()
    table[...] = mm(feat_in[...], weight_in[...]).astype(BF16)
    gather_slots(counts, send_in, table, out, chunk_list)


def side_gather_kernel(cols, counts, recv, feat, weight, bias, out, table, *chunk_list):
    table[...] = (mm(feat[...], weight[:, cols]) + bias[:, cols]).astype(BF16)
    gather_slots(counts, recv, table, out, chunk_list)


def back_gather_kernel(cols, counts, recv, cot, weight, out, table, *chunk_list):
    table[...] = mm_nt(cot[...], weight[cols, :]).astype(BF16)
    gather_slots(counts, recv, table, out, chunk_list)


def near_hot(index_row, rows):
    spread = down_rows(index_row)
    lane = lax.broadcasted_iota(jnp.int32, spread.shape, 1)
    return as_hot(spread == jnp.where(lane < rows, lane, lane - rows))


def edge_groups(counts, index_ref, flips, side, total, outs, chunk_list, edges):
    rows = total.shape[1]
    ours = len(outs) == 1
    blocks = [k for k in range(9) if (k % 3 == 1) == ours]
    groups = list_chunks(counts, index_ref.shape[2], *chunk_list, blocks=blocks)
    total[...] = jnp.zeros(total.shape, F32)

    def body(chunks):
        places = [place_of(k, flips) - (0 if ours else 3) for k, _, _ in chunks]
        index_rows = [rows_of(index_ref, chunk) for chunk in chunks]

        def gather(j):
            return mm(near_hot(index_rows[j], rows)[:, : side.shape[1]], side[places[j]])

        received = gather(0)
        for j, chunk in enumerate(chunks):
            following = gather(j + 1) if j + 1 < len(chunks) else None
            value = edges(chunk, received)
            total[places[j]] += mm(scatter_hot(index_rows[j], rows, chunk[2]), value)
            received = following

    each_group(groups, chunk_list, body)
    for place, out in enumerate(outs):
        out[...] = total[3 * place : 3 * place + 3].astype(BF16)


def stack_near(nears, side):
    for place, tiles in enumerate(nears):
        side[3 * place : 3 * place + 3] = tiles[...]


def enc_forward_kernel(n, counts, flips, recv, *refs):
    nears, (weight, bias, sent), refs = refs[:n], refs[n : n + 3], refs[n + 3 + (n == 1) :]
    outs, (slope, side, total, *chunk_list) = refs[:n], refs[n:]
    rows = total.shape[1]
    for place, near in enumerate(nears):
        feats = near[...].reshape(3 * rows, near.shape[2])
        exact = mm(feats, weight[...]) + bias[...]
        high = exact.astype(BF16)
        low = (exact - high.astype(F32)).astype(BF16)
        side[3 * place : 3 * place + 3, :rows, :] = high.reshape(3, rows, -1)
        side[3 * place : 3 * place + 3, rows:, :] = low.reshape(3, rows, -1)

    def edges(chunk, received):
        k, at, _ = chunk
        pre = sent[k, pl.ds(at, CHUNK), :].astype(F32) + received
        squashed = gate(pre)
        message = pre * squashed
        slope[k, pl.ds(at, CHUNK), :] = (squashed + message * (1.0 - squashed)).astype(BF16)
        return message.astype(BF16)

    edge_groups(counts, recv, flips, side, total, outs, chunk_list, edges)


def halves(lower, upper, at):
    return jnp.concatenate([lower[at], upper[at]], axis=1).astype(F32)


def dec_kernel(n, counts, flips, send, *refs):
    nears, tables, refs = refs[:n], refs[n : n + 4], refs[n + 4 + 2 * (n == 1) :]
    outs, (messages, grads, near, total, *chunk_list) = refs[:n], refs[n:]
    stack_near(nears, near)

    def edges(chunk, received):
        k, at, _ = chunk
        here = (k, pl.ds(at, CHUNK), slice(None))
        pre = halves(*tables[:2], here) + received
        squashed = gate(pre)
        message = pre * squashed
        messages[here] = message.astype(BF16)
        slope = squashed + message * (1.0 - squashed)
        grad = (halves(*tables[2:], here) * slope).astype(BF16)
        grads[here] = grad
        return grad

    edge_groups(counts, send, flips, near, total, outs, chunk_list, edges)


def enc_backward_kernel(n, counts, flips, recv, *refs):
    nears, slope, refs = refs[:n], refs[n], refs[n + 1 + (n == 1) :]
    outs, (grads, near, total, *chunk_list) = refs[:n], refs[n:]
    stack_near(nears, near)

    def edges(chunk, received):
        k, at, _ = chunk
        here = (k, pl.ds(at, CHUNK), slice(None))
        grad = (received * slope[here].astype(F32)).astype(BF16)
        grads[here] = grad
        return grad

    edge_groups(counts, recv, flips, near, total, outs, chunk_list, edges)


def scatter_slots(counts, index_ref, values, total, chunk_list, cols=slice(None)):
    groups = list_chunks(counts, index_ref.shape[2], *chunk_list)
    total[...] = jnp.zeros(total.shape, F32)

    def body(chunks):
        hots = [scatter_hot(rows_of(index_ref, c), total.shape[0], c[2]) for c in chunks]
        rows = [values[k, pl.ds(at, CHUNK), cols] for k, at, _ in chunks]
        total[...] += mm(jnp.concatenate(hots, axis=1), jnp.concatenate(rows, axis=0))

    each_group(groups, chunk_list, body)


def scatter_kernel(cols, counts, index_ref, values, out, total, *chunk_list):
    scatter_slots(counts, index_ref, values, total, chunk_list, cols)
    out[...] = total[...].astype(BF16)


def grid_new_kernel(
    cols, counts, recv, messages, feat, lower, weight, out, total, *chunk_list
):
    scatter_slots(counts, recv, messages, total, chunk_list, cols)
    half = lower.shape[1]
    update = mm(lower[...], weight[:half, :]) + mm(total[...].astype(BF16), weight[half:, :])
    out[...] = (feat[...].astype(F32) + update).astype(BF16)


def dec_grid_kernel(
    cols, counts, recv, grads, cot, lower, weight, out, total, *chunk_list
):
    scatter_slots(counts, recv, grads, total, chunk_list, cols)
    half = lower.shape[1]
    back = mm_nt(lower[...], weight[:, :half])
    back += mm_nt(total[...].astype(BF16), weight[:, half:])
    out[...] = cot[...].astype(F32) + back


def grid_grad_kernel(counts, send, grads, partial, weight, out, total, *chunk_list):
    scatter_slots(counts, send, grads, total, chunk_list)
    back = mm_nt(total[...].astype(BF16), weight[...])
    out[...] = (partial[...] + back).astype(BF16)


def fold_kernel(own, east, west, kept, to_first, to_second):
    total = own[...].astype(F32) + east[...].astype(F32) + west[...].astype(F32)
    kept[...] = total[0]
    to_first[...] = total[1].astype(BF16)
    to_second[...] = total[2].astype(BF16)


def mesh_new_kernel(kept, first, second, feat, out_weight, weight, proj):
    summed = kept[...] + first[...].astype(F32) + second[...].astype(F32)
    update = mm(summed.astype(BF16), out_weight[...])
    proj[...] = mm((feat[...].astype(F32) + update).astype(BF16), weight[...]).astype(BF16)


def mesh_back_kernel(kept, first, second, weight, out_weight, back, enc_back):
    summed = kept[...] + first[...].astype(F32) + second[...].astype(F32)
    exact = mm_nt(summed.astype(BF16), weight[...])
    back[...] = exact
    enc_back[...] = mm_nt(exact.astype(BF16), out_weight[...]).astype(BF16)


def mesh_grad_kernel(kept, first, second, back, weight, out):
    summed = kept[...] + first[...].astype(F32) + second[...].astype(F32)
    out[...] = (back[...] + mm_nt(summed.astype(BF16), weight[...])).astype(BF16)


def along(axis, pairs):
    return lambda value: lax.ppermute(value, axis, pairs)


def swaps(size, start):
    edges = [(i, (i + 1) % size) for i in range(start, size, 2)]
    return edges + [(j, i) for i, j in edges]


def on_device(
    grid_feat, mesh_feat, enc_send, enc_recv, enc_count, dec_send, dec_recv, dec_count,
    enc_src, enc_dst, enc_bias, enc_out, dec_src, dec_dst, dec_bias, dec_out, grid_cot,
):
    grid_rows, width = grid_feat.shape
    mesh_rows = mesh_feat.shape[0]
    cap_e = enc_send.shape[2]
    cap_d = dec_send.shape[2]
    lat_size = lax.axis_size("lat")
    lon_size = lax.axis_size("lon")
    flips = jnp.stack([lax.rem(lax.axis_index(a), 2) for a in ("lat", "lon")]).astype(jnp.int32)
    lat_first, lat_second = (along("lat", swaps(lat_size, i)) for i in range(2))
    lon_first, lon_second = (along("lon", swaps(lon_size, i)) for i in range(2))

    def spread(local_tile):
        pieces = [local_tile, lat_first(local_tile), lat_second(local_tile)]
        three = jnp.stack(pieces)
        return three, lon_first(three), lon_second(three)

    def fold(own, to_first, to_second):
        arrived = lon_first(to_first), lon_second(to_second)
        kept, to_first, to_second = kernel(
            fold_kernel, [exact_tile, tile, tile], [], own, *arrived, smem=0
        )
        return kept, lat_first(to_first), lat_second(to_second)

    def kernel(body, outs, scratch, *args, smem=1, mib=12, work=0, specs=None, alias=()):
        return pl.pallas_call(
            body,
            out_shape=outs,
            in_specs=specs or [SMEM] * smem + [VMEM] * (len(args) - smem),
            input_output_aliases=dict(alias),
            out_specs=[VMEM] * len(outs),
            scratch_shapes=scratch,
            compiler_params=pltpu.CompilerParams(vmem_limit_bytes=mib * 1024 * 1024),
            cost_estimate=pl.CostEstimate(flops=work, bytes_accessed=0, transcendentals=0),
        )(*args)

    def array(*shape):
        return jax.ShapeDtypeStruct(shape, BF16)

    tile = array(mesh_rows, width)
    exact_tile = jax.ShapeDtypeStruct((mesh_rows, width), F32)
    three = [array(3, mesh_rows, width)] * 3
    enc_slots = [array(9, cap_e, width)]
    dec_slots = [array(9, cap_d, width)]
    grid_tile = [array(grid_rows, width)]
    chunk_list = [pltpu.SMEM((9 * cap_d // CHUNK + GROUP,), jnp.int32)] * 3
    lower, upper = slice(0, width // 2), slice(width // 2, width)
    half_grid = [array(grid_rows, width // 2)]
    half_slots = [array(9, cap_d, width // 2)]
    rounded_half = [pltpu.VMEM((grid_rows, width // 2), BF16)] + chunk_list
    exact_half = [pltpu.VMEM((grid_rows, width // 2), F32)] + chunk_list
    rounded_grid = [pltpu.VMEM((grid_rows, width), BF16)] + chunk_list
    near = (mesh_rows, width), BF16
    near_split = (2 * mesh_rows, width), BF16
    near_total = (mesh_rows, width), F32
    enc_work = 2 * grid_rows * width * 9 * cap_e
    dec_work = 2 * grid_rows * width * 9 * cap_d

    enc_send, enc_recv, dec_send, dec_recv = (
        jnp.swapaxes(a, 0, 1) for a in (enc_send, enc_recv, dec_send, dec_recv)
    )

    near_feat = spread(mesh_feat)
    (sent,) = kernel(
        enc_gather_kernel, enc_slots,
        [
            rounded_grid[0],
            pltpu.VMEM((9, 1, cap_e), jnp.int32),
            pltpu.VMEM((grid_rows, width), BF16),
            pltpu.VMEM((width, width), BF16),
            pltpu.SemaphoreType.DMA((3,)),
            *chunk_list,
        ],
        *(
            pltpu.with_memory_space_constraint(a, pltpu.HBM)
            for a in (enc_count, enc_send, grid_feat, enc_src)
        ),
        work=enc_work, specs=[SMEM, HBM, HBM, HBM],
    )
    back_at = [
        kernel(
            functools.partial(back_gather_kernel, cols), half_slots, rounded_half,
            dec_count, dec_recv, grid_cot, dec_out, work=dec_work // 2,
        )[0]
        for cols in (lower, upper)
    ]
    side_at = [
        kernel(
            functools.partial(side_gather_kernel, cols), half_slots, rounded_half,
            dec_count, dec_recv, grid_feat, dec_dst, dec_bias.reshape(1, width),
            work=dec_work // 2,
        )[0]
        for cols in (lower, upper)
    ]

    def edges(body, counts, index, nears, extra, slots, scratch, work):
        outs = []
        fill = []
        for n in (2, 1):
            args = (counts, flips, index, *(nears[1:] if n == 2 else nears[:1]), *extra, *fill)
            base = len(args) - len(fill)
            made = kernel(
                functools.partial(body, n), three[:n] + slots,
                [pltpu.VMEM((3 * n,) + shape, kind) for shape, kind in scratch] + chunk_list,
                *args, smem=2, work=n * work // 3,
                alias=[(base + i, n + i) for i in range(len(fill))],
            )
            outs = list(made[:n]) + outs
            fill = made[n:]
        return outs, fill

    enc_partial, (slope,) = edges(
        enc_forward_kernel, enc_count, enc_recv, near_feat,
        (enc_dst, enc_bias.reshape(1, width), sent), enc_slots, [near_split, near_total],
        enc_work // 4,
    )
    (dec_proj,) = kernel(
        mesh_new_kernel, [tile], [],
        *fold(*enc_partial), mesh_feat, enc_out, dec_src, smem=0,
    )

    dec_partial, (messages, dec_grads) = edges(
        dec_kernel, dec_count, dec_send, spread(dec_proj),
        (*side_at, *back_at), dec_slots * 2, [near, near_total], dec_work // 4,
    )
    mesh_back, enc_back = kernel(
        mesh_back_kernel, [exact_tile, tile], [],
        *fold(*dec_partial), dec_src, enc_out, smem=0,
    )

    (sum_lower,) = kernel(
        functools.partial(scatter_kernel, lower), half_grid, exact_half,
        dec_count, dec_recv, messages, work=dec_work // 2,
    )
    (grid_new,) = kernel(
        functools.partial(grid_new_kernel, upper), grid_tile, exact_half,
        dec_count, dec_recv, messages, grid_feat, sum_lower, dec_out, work=dec_work // 2,
    )
    (local_lower,) = kernel(
        functools.partial(scatter_kernel, lower), half_grid, exact_half,
        dec_count, dec_recv, dec_grads, work=dec_work // 2,
    )
    (dec_grid,) = kernel(
        functools.partial(dec_grid_kernel, upper),
        [jax.ShapeDtypeStruct((grid_rows, width), F32)], exact_half,
        dec_count, dec_recv, dec_grads, grid_cot, local_lower, dec_dst, work=dec_work // 2,
    )

    grad_partial, (grads,) = edges(
        enc_backward_kernel, enc_count, enc_recv, spread(enc_back),
        (slope,), enc_slots, [near, near_total], enc_work // 4,
    )
    (mesh_grad,) = kernel(
        mesh_grad_kernel, [tile], [],
        *fold(*grad_partial), mesh_back, enc_dst, smem=0,
    )

    (grid_grad,) = kernel(
        grid_grad_kernel, grid_tile,
        [pltpu.VMEM((grid_rows, width), F32)] + chunk_list,
        enc_count, enc_send, grads, dec_grid, enc_src, work=enc_work,
    )
    return grid_new, mesh_grad, grid_grad


def solution(mesh):
    rows = P(("lat", "lon"), None)
    edges = P(("lat", "lon"), None, None)
    return jax.shard_map(
        on_device,
        mesh=mesh,
        in_specs=(rows, rows, edges, edges, rows, edges, edges, rows)
        + (P(),) * 8
        + (rows,),
        out_specs=(rows, rows, rows),
        check_vma=False,
    )
```

```python
import functools

import jax
import jax.numpy as jnp
from jax import lax
from jax.experimental import pallas as pl
from jax.experimental.pallas import tpu as pltpu
from jax.sharding import PartitionSpec as P


F32 = jnp.float32
BF16 = jnp.bfloat16
LANES = 128
CHUNK = 128
GROUP = 4

HBM = pl.BlockSpec(memory_space=pltpu.HBM)
VMEM = pl.BlockSpec(memory_space=pltpu.VMEM)
SMEM = pl.BlockSpec(memory_space=pltpu.SMEM)


def mm(lhs, rhs):
    return jnp.dot(lhs, rhs, preferred_element_type=F32)


def mm_nt(lhs, rhs):
    return lax.dot_general(lhs, rhs, (((1,), (1,)), ((), ())), preferred_element_type=F32)


def as_hot(mask):
    return jnp.where(mask, 1.0, 0.0).astype(BF16)


def down_rows(index_row):
    return jnp.transpose(jnp.broadcast_to(index_row, (LANES, index_row.shape[1])))


def gather_hot(index_row, rows):
    spread = down_rows(index_row)
    lane = lax.broadcasted_iota(jnp.int32, spread.shape, 1)
    return jnp.concatenate(
        [as_hot(spread == lane + start) for start in range(0, rows, LANES)], axis=1
    )


def scatter_hot(index_row, rows, live):
    slots = index_row.shape[1]
    slot = lax.broadcasted_iota(jnp.int32, (1, slots), 1)
    index_row = jnp.where(slot < live, index_row, -1)
    return as_hot(lax.broadcasted_iota(jnp.int32, (rows, slots), 0) == index_row)


def gate(pre):
    return 0.5 * jnp.tanh(0.5 * pre) + 0.5


def list_chunks(counts, capacity, block, start, live, blocks=range(9)):
    found = jnp.int32(0)
    for k in blocks:
        count = counts[0, k]
        for at in range(0, capacity, CHUNK):
            block[found] = k
            start[found] = at
            live[found] = count - at
            found += (count > at).astype(jnp.int32)
    last = jnp.maximum(found - 1, 0)
    for j in range(GROUP - 1):
        block[found + j] = block[last]
        start[found + j] = start[last]
        live[found + j] = 0
    return lax.div(found + (GROUP - 1), GROUP)


def each_group(groups, chunk_list, body):
    block, start, live = chunk_list

    @pl.loop(0, groups)
    def _(g):
        at = [GROUP * g + j for j in range(GROUP)]
        body([(block[n], pl.multiple_of(start[n], CHUNK), live[n]) for n in at])


def rows_of(index_ref, chunk):
    k, at, _ = chunk
    return index_ref[k, :, pl.ds(at, CHUNK)]


def place_of(k, flips):
    def place(offset, flip):
        return jnp.where(offset == 0, 0, jnp.where(offset == 1 - 2 * flip, 1, 2))

    return 3 * place(lax.rem(k, 3) - 1, flips[1]) + place(lax.div(k, 3) - 1, flips[0])


def gather_slots(counts, index_ref, table, out, chunk_list):
    groups = list_chunks(counts, index_ref.shape[2], *chunk_list)

    def body(chunks):
        hots = [gather_hot(rows_of(index_ref, c), table.shape[0]) for c in chunks]
        rows = mm(jnp.concatenate(hots, axis=0), table[...]).astype(BF16)
        for j, (k, at, _) in enumerate(chunks):
            out[k, pl.ds(at, CHUNK), :] = rows[j * CHUNK : (j + 1) * CHUNK]

    each_group(groups, chunk_list, body)


def enc_gather_kernel(
    counts, send, feat, weight, out, table, send_in, feat_in, weight_in, sems, *chunk_list
):
    pairs = ((feat, feat_in), (weight, weight_in), (send, send_in))
    copies = [pltpu.make_async_copy(a, b, sems.at[i]) for i, (a, b) in enumerate(pairs)]
    for copy in copies:
        copy.start()
    for copy in copies:
        copy.wait()
    table[...] = mm(feat_in[...], weight_in[...]).astype(BF16)
    gather_slots(counts, send_in, table, out, chunk_list)


def side_gather_kernel(cols, counts, recv, feat, weight, bias, out, table, *chunk_list):
    table[...] = (mm(feat[...], weight[:, cols]) + bias[:, cols]).astype(BF16)
    gather_slots(counts, recv, table, out, chunk_list)


def back_gather_kernel(cols, counts, recv, cot, weight, out, table, *chunk_list):
    table[...] = mm_nt(cot[...], weight[cols, :]).astype(BF16)
    gather_slots(counts, recv, table, out, chunk_list)


def near_hot(index_row, rows):
    spread = down_rows(index_row)
    lane = lax.broadcasted_iota(jnp.int32, spread.shape, 1)
    return as_hot(spread == jnp.where(lane < rows, lane, lane - rows))


def edge_groups(counts, index_ref, flips, side, total, outs, chunk_list, edges):
    rows = total.shape[1]
    ours = len(outs) == 1
    blocks = [k for k in range(9) if (k % 3 == 1) == ours]
    groups = list_chunks(counts, index_ref.shape[2], *chunk_list, blocks=blocks)
    total[...] = jnp.zeros(total.shape, F32)

    def body(chunks):
        places = [place_of(k, flips) - (0 if ours else 3) for k, _, _ in chunks]
        index_rows = [rows_of(index_ref, chunk) for chunk in chunks]

        def gather(j):
            return mm(near_hot(index_rows[j], rows)[:, : side.shape[1]], side[places[j]])

        received = gather(0)
        for j, chunk in enumerate(chunks):
            following = gather(j + 1) if j + 1 < len(chunks) else None
            value = edges(chunk, received)
            total[places[j]] += mm(scatter_hot(index_rows[j], rows, chunk[2]), value)
            received = following

    each_group(groups, chunk_list, body)
    for place, out in enumerate(outs):
        out[...] = total[3 * place : 3 * place + 3].astype(BF16)


def stack_near(nears, side):
    for place, tiles in enumerate(nears):
        side[3 * place : 3 * place + 3] = tiles[...]


def enc_forward_kernel(n, counts, flips, recv, *refs):
    nears, (weight, bias, sent), refs = refs[:n], refs[n : n + 3], refs[n + 3 + (n == 1) :]
    outs, (slope, side, total, *chunk_list) = refs[:n], refs[n:]
    rows = total.shape[1]
    for place, near in enumerate(nears):
        feats = near[...].reshape(3 * rows, near.shape[2])
        exact = mm(feats, weight[...]) + bias[...]
        high = exact.astype(BF16)
        low = (exact - high.astype(F32)).astype(BF16)
        side[3 * place : 3 * place + 3, :rows, :] = high.reshape(3, rows, -1)
        side[3 * place : 3 * place + 3, rows:, :] = low.reshape(3, rows, -1)

    def edges(chunk, received):
        k, at, _ = chunk
        pre = sent[k, pl.ds(at, CHUNK), :].astype(F32) + received
        squashed = gate(pre)
        message = pre * squashed
        slope[k, pl.ds(at, CHUNK), :] = (squashed + message * (1.0 - squashed)).astype(BF16)
        return message.astype(BF16)

    edge_groups(counts, recv, flips, side, total, outs, chunk_list, edges)


def halves(lower, upper, at):
    return jnp.concatenate([lower[at], upper[at]], axis=1).astype(F32)


def dec_kernel(n, counts, flips, send, *refs):
    nears, tables, refs = refs[:n], refs[n : n + 4], refs[n + 4 + 2 * (n == 1) :]
    outs, (messages, grads, near, total, *chunk_list) = refs[:n], refs[n:]
    stack_near(nears, near)

    def edges(chunk, received):
        k, at, _ = chunk
        here = (k, pl.ds(at, CHUNK), slice(None))
        pre = halves(*tables[:2], here) + received
        squashed = gate(pre)
        message = pre * squashed
        messages[here] = message.astype(BF16)
        slope = squashed + message * (1.0 - squashed)
        grad = (halves(*tables[2:], here) * slope).astype(BF16)
        grads[here] = grad
        return grad

    edge_groups(counts, send, flips, near, total, outs, chunk_list, edges)


def enc_backward_kernel(n, counts, flips, recv, *refs):
    nears, slope, refs = refs[:n], refs[n], refs[n + 1 + (n == 1) :]
    outs, (grads, near, total, *chunk_list) = refs[:n], refs[n:]
    stack_near(nears, near)

    def edges(chunk, received):
        k, at, _ = chunk
        here = (k, pl.ds(at, CHUNK), slice(None))
        grad = (received * slope[here].astype(F32)).astype(BF16)
        grads[here] = grad
        return grad

    edge_groups(counts, recv, flips, near, total, outs, chunk_list, edges)


def scatter_slots(
    counts, index_ref, values, total, chunk_list, cols=slice(None), blocks=range(9), first=None
):
    groups = list_chunks(counts, index_ref.shape[2], *chunk_list, blocks=blocks)
    total[...] = jnp.zeros(total.shape, F32) if first is None else first[...]

    def body(chunks):
        hots = [scatter_hot(rows_of(index_ref, c), total.shape[0], c[2]) for c in chunks]
        rows = [values[k, pl.ds(at, CHUNK), cols] for k, at, _ in chunks]
        total[...] += mm(jnp.concatenate(hots, axis=1), jnp.concatenate(rows, axis=0))

    each_group(groups, chunk_list, body)


def scatter_kernel(cols, counts, index_ref, values, out, total, *chunk_list):
    scatter_slots(counts, index_ref, values, total, chunk_list, cols)
    out[...] = total[...].astype(BF16)


def grid_new_kernel(
    cols, counts, recv, messages, feat, lower, weight, out, total, *chunk_list
):
    scatter_slots(counts, recv, messages, total, chunk_list, cols)
    half = lower.shape[1]
    update = mm(lower[...], weight[:half, :]) + mm(total[...].astype(BF16), weight[half:, :])
    out[...] = (feat[...].astype(F32) + update).astype(BF16)


def dec_grid_kernel(counts, recv, grads, cot, weight, out, total, *chunk_list):
    scatter_slots(counts, recv, grads, total, chunk_list)
    out[...] = cot[...].astype(F32) + mm_nt(total[...].astype(BF16), weight[...])


def partner_total_kernel(counts, send, grads, out, *chunk_list):
    partners = [k for k in range(9) if k % 3 != 1]
    scatter_slots(counts, send, grads, out, chunk_list, blocks=partners)


def grid_grad_kernel(counts, send, grads, first, partial, weight, out, total, *chunk_list):
    scatter_slots(counts, send, grads, total, chunk_list, blocks=(1, 4, 7), first=first)
    back = mm_nt(total[...].astype(BF16), weight[...])
    out[...] = (partial[...] + back).astype(BF16)


def fold_kernel(own, east, west, kept, to_first, to_second):
    total = own[...].astype(F32) + east[...].astype(F32) + west[...].astype(F32)
    kept[...] = total[0]
    to_first[...] = total[1].astype(BF16)
    to_second[...] = total[2].astype(BF16)


def mesh_new_kernel(kept, first, second, feat, out_weight, weight, proj):
    summed = kept[...] + first[...].astype(F32) + second[...].astype(F32)
    update = mm(summed.astype(BF16), out_weight[...])
    proj[...] = mm((feat[...].astype(F32) + update).astype(BF16), weight[...]).astype(BF16)


def mesh_back_kernel(kept, first, second, weight, out_weight, back, enc_back):
    summed = kept[...] + first[...].astype(F32) + second[...].astype(F32)
    exact = mm_nt(summed.astype(BF16), weight[...])
    back[...] = exact
    enc_back[...] = mm_nt(exact.astype(BF16), out_weight[...]).astype(BF16)


def mesh_grad_kernel(kept, first, second, back, weight, out):
    summed = kept[...] + first[...].astype(F32) + second[...].astype(F32)
    out[...] = (back[...] + mm_nt(summed.astype(BF16), weight[...])).astype(BF16)


def along(axis, pairs):
    return lambda value: lax.ppermute(value, axis, pairs)


def swaps(size, start):
    edges = [(i, (i + 1) % size) for i in range(start, size, 2)]
    return edges + [(j, i) for i, j in edges]


def on_device(
    grid_feat, mesh_feat, enc_send, enc_recv, enc_count, dec_send, dec_recv, dec_count,
    enc_src, enc_dst, enc_bias, enc_out, dec_src, dec_dst, dec_bias, dec_out, grid_cot,
):
    grid_rows, width = grid_feat.shape
    mesh_rows = mesh_feat.shape[0]
    cap_e = enc_send.shape[2]
    cap_d = dec_send.shape[2]
    lat_size = lax.axis_size("lat")
    lon_size = lax.axis_size("lon")
    flips = jnp.stack([lax.rem(lax.axis_index(a), 2) for a in ("lat", "lon")]).astype(jnp.int32)
    lat_first, lat_second = (along("lat", swaps(lat_size, i)) for i in range(2))
    lon_first, lon_second = (along("lon", swaps(lon_size, i)) for i in range(2))

    def spread(local_tile):
        pieces = [local_tile, lat_first(local_tile), lat_second(local_tile)]
        three = jnp.stack(pieces)
        return three, lon_first(three), lon_second(three)

    def fold(own, to_first, to_second):
        arrived = lon_first(to_first), lon_second(to_second)
        kept, to_first, to_second = kernel(
            fold_kernel, [exact_tile, tile, tile], [], own, *arrived, smem=0
        )
        return kept, lat_first(to_first), lat_second(to_second)

    def kernel(body, outs, scratch, *args, smem=1, mib=12, work=0, specs=None, alias=()):
        return pl.pallas_call(
            body,
            out_shape=outs,
            in_specs=specs or [SMEM] * smem + [VMEM] * (len(args) - smem),
            input_output_aliases=dict(alias),
            out_specs=[VMEM] * len(outs),
            scratch_shapes=scratch,
            compiler_params=pltpu.CompilerParams(vmem_limit_bytes=mib * 1024 * 1024),
            cost_estimate=pl.CostEstimate(flops=work, bytes_accessed=0, transcendentals=0),
        )(*args)

    def array(*shape):
        return jax.ShapeDtypeStruct(shape, BF16)

    tile = array(mesh_rows, width)
    exact_tile = jax.ShapeDtypeStruct((mesh_rows, width), F32)
    three = [array(3, mesh_rows, width)] * 3
    enc_slots = [array(9, cap_e, width)]
    dec_slots = [array(9, cap_d, width)]
    grid_tile = [array(grid_rows, width)]
    chunk_list = [pltpu.SMEM((9 * cap_d // CHUNK + GROUP,), jnp.int32)] * 3
    lower, upper = slice(0, width // 2), slice(width // 2, width)
    half_grid = [array(grid_rows, width // 2)]
    half_slots = [array(9, cap_d, width // 2)]
    rounded_half = [pltpu.VMEM((grid_rows, width // 2), BF16)] + chunk_list
    exact_half = [pltpu.VMEM((grid_rows, width // 2), F32)] + chunk_list
    rounded_grid = [pltpu.VMEM((grid_rows, width), BF16)] + chunk_list
    near = (mesh_rows, width), BF16
    near_split = (2 * mesh_rows, width), BF16
    near_total = (mesh_rows, width), F32
    exact_grid = [pltpu.VMEM((grid_rows, width), F32)] + chunk_list
    exact_tile_grid = [jax.ShapeDtypeStruct((grid_rows, width), F32)]
    enc_work = 2 * grid_rows * width * 9 * cap_e
    dec_work = 2 * grid_rows * width * 9 * cap_d

    enc_send, enc_recv, dec_send, dec_recv = (
        jnp.swapaxes(a, 0, 1) for a in (enc_send, enc_recv, dec_send, dec_recv)
    )

    near_feat = spread(mesh_feat)
    (sent,) = kernel(
        enc_gather_kernel, enc_slots,
        [
            rounded_grid[0],
            pltpu.VMEM((9, 1, cap_e), jnp.int32),
            pltpu.VMEM((grid_rows, width), BF16),
            pltpu.VMEM((width, width), BF16),
            pltpu.SemaphoreType.DMA((3,)),
            *chunk_list,
        ],
        *(
            pltpu.with_memory_space_constraint(a, pltpu.HBM)
            for a in (enc_count, enc_send, grid_feat, enc_src)
        ),
        work=enc_work, specs=[SMEM, HBM, HBM, HBM],
    )
    back_at = [
        kernel(
            functools.partial(back_gather_kernel, cols), half_slots, rounded_half,
            dec_count, dec_recv, grid_cot, dec_out, work=dec_work // 2,
        )[0]
        for cols in (lower, upper)
    ]
    side_at = [
        kernel(
            functools.partial(side_gather_kernel, cols), half_slots, rounded_half,
            dec_count, dec_recv, grid_feat, dec_dst, dec_bias.reshape(1, width),
            work=dec_work // 2,
        )[0]
        for cols in (lower, upper)
    ]

    def edges(body, counts, index, nears, extra, slots, scratch, work):
        outs = []
        fill = []
        for n in (2, 1):
            args = (counts, flips, index, *(nears[1:] if n == 2 else nears[:1]), *extra, *fill)
            base = len(args) - len(fill)
            made = kernel(
                functools.partial(body, n), three[:n] + slots,
                [pltpu.VMEM((3 * n,) + shape, kind) for shape, kind in scratch] + chunk_list,
                *args, smem=2, work=n * work // 3,
                alias=[(base + i, n + i) for i in range(len(fill))],
            )
            outs = list(made[:n]) + outs
            fill = made[n:]
        return outs, fill

    enc_partial, (slope,) = edges(
        enc_forward_kernel, enc_count, enc_recv, near_feat,
        (enc_dst, enc_bias.reshape(1, width), sent), enc_slots, [near_split, near_total],
        enc_work // 4,
    )
    (dec_proj,) = kernel(
        mesh_new_kernel, [tile], [],
        *fold(*enc_partial), mesh_feat, enc_out, dec_src, smem=0,
    )

    dec_partial, (messages, dec_grads) = edges(
        dec_kernel, dec_count, dec_send, spread(dec_proj),
        (*side_at, *back_at), dec_slots * 2, [near, near_total], dec_work // 4,
    )
    mesh_back, enc_back = kernel(
        mesh_back_kernel, [exact_tile, tile], [],
        *fold(*dec_partial), dec_src, enc_out, smem=0,
    )

    (sum_lower,) = kernel(
        functools.partial(scatter_kernel, lower), half_grid, exact_half,
        dec_count, dec_recv, messages, work=dec_work // 2,
    )
    (grid_new,) = kernel(
        functools.partial(grid_new_kernel, upper), grid_tile, exact_half,
        dec_count, dec_recv, messages, grid_feat, sum_lower, dec_out, work=dec_work // 2,
    )
    (dec_grid,) = kernel(
        dec_grid_kernel, exact_tile_grid, exact_grid,
        dec_count, dec_recv, dec_grads, grid_cot, dec_dst, work=dec_work,
    )

    grad_partial, (grads,) = edges(
        enc_backward_kernel, enc_count, enc_recv, spread(enc_back),
        (slope,), enc_slots, [near, near_total], enc_work // 4,
    )
    (mesh_grad,) = kernel(
        mesh_grad_kernel, [tile], [],
        *fold(*grad_partial), mesh_back, enc_dst, smem=0,
    )

    (partner_total,) = kernel(
        partner_total_kernel, exact_tile_grid, chunk_list,
        enc_count, enc_send, grads, work=2 * enc_work // 3,
    )
    (grid_grad,) = kernel(
        grid_grad_kernel, grid_tile, exact_grid,
        enc_count, enc_send, grads, partner_total, dec_grid, enc_src, work=enc_work // 3,
    )
    return grid_new, mesh_grad, grid_grad


def solution(mesh):
    rows = P(("lat", "lon"), None)
    edges = P(("lat", "lon"), None, None)
    return jax.shard_map(
        on_device,
        mesh=mesh,
        in_specs=(rows, rows, edges, edges, rows, edges, edges, rows)
        + (P(),) * 8
        + (rows,),
        out_specs=(rows, rows, rows),
        check_vma=False,
    )
```
